32 devices in a mesh: day: 8 (over y, x, core), pair: 4 (over z).
Axes of the slice: x: 2, y: 2, z: 4, core: 2. Of those that a mesh axis runs over, the one named last changes fastest.
Arguments:
- correlations: bfloat16 [32, 2048, 2001], P('day', 'pair'), may hold values from -8 to 8
- mask: int32 [32, 2048], P('day', 'pair'), may hold values from 0 to 1, as said below
- counts: int32 [2048], P(('pair', 'day')), may hold values from 1 to 32, as said below
Outputs:
- phase_weighted: float32 [2048, 2001], P(('pair', 'day'))
- linear: float32 [2048, 2001], P(('pair', 'day'))
The draws below stay inside these ranges and needn't reach their ends.
Inputs may be any that keep to these rules, and one draw needn't show every extreme that they name: `mask`: every pair has a usable correlation on at least one day. counts[p] equals the number of days d with mask[d, p] = 1.
All inputs are finite; a program needn't handle non-finite values.
Results may differ from the reference program's by a relative error of at most 0.00044.
Values may be sent and summed in bfloat16 or wider, within the bound.
A program may use at most 128 MiB of HBM per device.

```python
import jax
import jax.numpy as jnp
from jax import lax

LAGS = 2001
DAYS = 32
PAIRS = 2048


def mask_pair(key):
    base = jax.random.fold_in(key, 7)
    keys = jax.random.split(base, 5)
    day_rate = jax.random.randint(keys[0], (DAYS,), 30, 101)
    pair_rate = jax.random.randint(keys[1], (PAIRS,), 40, 101)
    draws = jax.random.randint(keys[2], (DAYS, PAIRS), 0, 10000)
    usable = (draws < day_rate[:, None] * pair_rate[None, :]).astype(jnp.int32)
    forced = jax.random.randint(keys[3], (PAIRS,), 0, DAYS)
    chosen = (jnp.arange(DAYS)[:, None] == forced[None, :]).astype(jnp.int32)
    usable = jnp.maximum(usable, chosen)
    full_pair = jax.random.randint(keys[4], (), 0, PAIRS)
    always = (jnp.arange(PAIRS) == full_pair).astype(jnp.int32)
    usable = jnp.maximum(usable, always[None, :])
    return (usable, jnp.sum(usable, axis=0).astype(jnp.int32))


def draw_mask(key, part):
    return mask_pair(key)[0]


def draw_counts(key, part):
    return mask_pair(key)[1]


def draw_correlations(key, part):
    keys = jax.random.split(jax.random.fold_in(key, 3), 5)
    block_index = jnp.arange(PAIRS) // 64
    block_total = (PAIRS + 63) // 64
    pair_scale = jnp.exp(jax.random.uniform(keys[0], (PAIRS,), jnp.float32, -0.8, 0.8))
    block_scale = jnp.exp(jax.random.uniform(keys[1], (block_total,), jnp.float32, -0.8, 0.8))[block_index]
    day_scale = jnp.exp(jax.random.uniform(keys[2], (DAYS,), jnp.float32, -0.7, 0.7))
    signal = 0.7 * jax.random.normal(keys[3], (PAIRS, LAGS), jnp.float32)
    noise = jax.random.normal(keys[4], (DAYS, PAIRS, LAGS), jnp.float32)
    values = day_scale[:, None, None] * (pair_scale * block_scale)[None, :, None] * (signal[None] + noise)
    return jnp.clip(values, -8.0, 8.0).astype(jnp.bfloat16)


def setup_inputs(seed: int = 0) -> dict:
    seeds = jax.random.split(jax.random.key(seed), 4)
    correlations = draw_correlations(jax.random.fold_in(seeds[3], 71), 0)
    mask = draw_mask(jax.random.fold_in(seeds[3], 71), 0)
    counts = draw_counts(jax.random.fold_in(seeds[3], 71), 0)
    return dict(correlations=correlations, mask=mask, counts=counts)


def hilbert_kernel():
    offset = jnp.arange(LAGS, dtype=jnp.int32)
    offset = jnp.where(offset > LAGS // 2, offset - LAGS, offset)
    phase_angle = jnp.pi * offset.astype(jnp.float32) / LAGS
    parity = 1.0 - 2.0 * (offset % 2).astype(jnp.float32)
    sine_safe = jnp.where(offset == 0, 1.0, jnp.sin(phase_angle))
    kernel = jnp.where(offset == 0, 0.0, (jnp.cos(phase_angle) - parity) / (LAGS * sine_safe))
    rounded = lax.optimization_barrier(kernel.astype(jnp.bfloat16))
    return rounded.astype(jnp.float32)

def hilbert_part(day_rows, kernel_spectrum):
    spectrum = jnp.fft.fft(day_rows, axis=-1)
    return jnp.real(jnp.fft.ifft(spectrum * kernel_spectrum, axis=-1))

def reference(correlations, mask, counts):
    masked = correlations * mask[:, :, None].astype(jnp.bfloat16)
    energy = lax.map(lambda day_rows: jnp.sum(jnp.square(day_rows.astype(jnp.float32))), masked)
    used_pairs = lax.optimization_barrier(jnp.sum(mask, axis=1)).astype(jnp.float32)
    weight = 1.0 / jnp.sqrt(energy / (LAGS * jnp.maximum(used_pairs, 1.0)) + 0.1)
    kernel_spectrum = jnp.fft.fft(hilbert_kernel())

    def add_day(totals, inputs):
        day_rows, day_weight = inputs
        values = day_rows.astype(jnp.float32)
        real_part = day_weight * values
        imag_part = day_weight * hilbert_part(values, kernel_spectrum)
        amplitude = jnp.sqrt(real_part * real_part + imag_part * imag_part + 0.25)
        return ((totals[0] + real_part, totals[1] + real_part / amplitude, totals[2] + imag_part / amplitude), None)
    zeros = jnp.zeros((PAIRS, LAGS), jnp.float32)
    totals, unused = lax.scan(add_day, (zeros, zeros, zeros), (masked, weight))
    divisor = jnp.maximum(counts.astype(jnp.float32), 1.0)[:, None]
    linear = totals[0] / divisor
    coherence = (totals[1] * totals[1] + totals[2] * totals[2]) / (divisor * divisor)
    return (linear * coherence, linear)
```

```python
import functools

import jax
import jax.numpy as jnp
import numpy as np
from jax import lax
from jax.experimental import pallas as pl
from jax.experimental.pallas import tpu as pltpu
from jax.sharding import PartitionSpec as P

TILE = 256
MESH = pl.DeviceIdType.MESH
FULL = 32767.0
UNIT = 2.0**20


def padded(lag_count):
    return -(-lag_count // TILE) * TILE


def kernel_strip(lag_count):
    f32 = np.float32
    offset = np.arange(lag_count, dtype=np.int32)
    offset = np.where(offset > lag_count // 2, offset - lag_count, offset)
    angle = f32(np.pi) * offset.astype(f32) / f32(lag_count)
    parity = f32(1) - f32(2) * (offset % 2).astype(f32)
    sine = np.where(offset == 0, f32(1), np.sin(angle)).astype(f32)
    kernel = np.where(offset == 0, f32(0), (np.cos(angle) - parity) / (f32(lag_count) * sine))
    width = padded(lag_count)
    index = np.arange(2 * width - TILE)[None, :] - np.arange(TILE)[:, None] - (width - TILE)
    return kernel.astype(f32)[index % lag_count].astype(jnp.bfloat16)


def codes(values):
    top = jnp.max(jnp.abs(values), axis=1, keepdims=True)
    units = (top * UNIT).astype(jnp.int32) + 1
    step = FULL * UNIT / units.astype(jnp.float32)
    return jnp.round(values * step).astype(jnp.int32), units


def join(high, low):
    return high * 65536 + (low & 65535)


def split(word):
    low = ((word & 65535) ^ 32768) - 32768
    return word >> 16, low


def stack_kernel(
    lag_count, x_hbm, mask_ref, strip_hbm, linear_ref, power_ref,
    rows_ref, stage, strip, table, sums, first_hilbert, mask_in, mask_turned, row_mask, day_weight,
    stat_out, stat_in, words_out, words_in,
    load_sem, stage_sem, strip_sem, swap_send, swap_recv, mask_send, mask_recv,
    stat_send, stat_recv, word_send, word_recv,
):
    width = table.shape[1]
    half = width // 2
    chips, all_days, owned, _ = rows_ref.shape
    days = all_days // 2
    total = all_days * owned
    part = owned // 2
    pieces = words_out.shape[0]
    peers = stat_in.shape[0]
    me, plane = lax.axis_index("day"), lax.axis_index("pair")
    chip, core = me // 2, me % 2
    partner = {"day": me ^ 1, "pair": plane}
    last = width - TILE
    tiles = [slice(j * TILE, min((j + 1) * TILE, lag_count)) for j in range(width // TILE)]

    def mine(g):
        return pltpu.make_async_copy(x_hbm.at[:, 2 * g + core], rows_ref.at[g, pl.ds(0, days)], load_sem.at[g])

    def staged(g):
        return pltpu.make_async_copy(x_hbm.at[:, 2 * g + 1 - core], stage.at[g], stage_sem.at[g])

    def swapped(g):
        return pltpu.make_async_remote_copy(
            stage.at[g], rows_ref.at[g, pl.ds(days, days)], swap_send.at[g], swap_recv.at[g],
            device_id=partner, device_id_type=MESH,
        )

    def peer(o):
        rank = (2 * plane + core + o) % (peers + 1)
        return {"day": 2 * chip + rank % 2, "pair": rank // 2}

    def told(o):
        return pltpu.make_async_remote_copy(
            stat_out, stat_in.at[o - 1], stat_send.at[o - 1], stat_recv.at[o - 1],
            device_id=peer(o), device_id_type=MESH,
        )

    def owner(o):
        return {"day": 2 * (chip ^ o) + core, "pair": plane}

    def shipped(piece, o):
        return pltpu.make_async_remote_copy(
            words_out.at[piece], words_in.at[piece], word_send.at[piece], word_recv.at[piece],
            device_id=owner(o), device_id_type=MESH,
        )

    far = range(chips - 1, 3, -1)
    order = [chip ^ o for o in (3, *far, 1, 2, 0)]
    strip_copy = pltpu.make_async_copy(strip_hbm, strip, strip_sem)
    strip_copy.start()
    for g in order:
        staged(g).start()
        mine(g).start()

    barrier = pltpu.get_barrier_semaphore()
    for o in range(1, peers + 1):
        pl.semaphore_signal(barrier, inc=1, device_id=peer(o), device_id_type=MESH)
    for o in range(1, chips):
        pl.semaphore_signal(barrier, inc=1, device_id=owner(o), device_id_type=MESH)
    strip_copy.wait()
    for i in range(width // TILE):
        start = width - TILE - i * TILE
        table[pl.ds(i * TILE, TILE), :] = strip[:, start : start + width]
    sums[:, :, last:] = jnp.zeros((3, owned, TILE), jnp.float32)
    pl.semaphore_wait(barrier, peers + chips - 1)

    mask_copy = pltpu.make_async_remote_copy(
        mask_ref, mask_in, mask_send, mask_recv, device_id=partner, device_id_type=MESH
    )
    mask_copy.start()
    for g in order:
        staged(g).wait()
        swapped(g).start()
    mask_copy.wait_recv()
    both_masks = jnp.concatenate([mask_ref[...], mask_in[...]], axis=0).astype(jnp.float32)
    mask_turned[...] = both_masks.T

    def mask_rows(block, count):
        rows = mask_turned[pl.ds(pl.multiple_of(block * owned, owned), owned), :]
        return jnp.concatenate([rows[:, d : d + 1] for d in range(count)], axis=0)

    def statistics(step, carry):
        g = chip ^ (chips - 1 - step)
        mine(g).wait()
        of_pairs = mask_rows(2 * g + core, all_days)
        row_mask[g] = of_pairs.reshape(all_days, owned, 1)
        for x_ref, rows in ((rows_ref.at[g, pl.ds(0, days)], of_pairs[: days * owned]),
                            (stage.at[g], mask_rows(2 * g + 1 - core, days))):
            x = x_ref[...].reshape(days * owned, lag_count).astype(jnp.float32)
            energy = jnp.sum(x * x, axis=1, keepdims=True) * rows
            both = jnp.concatenate(
                [jnp.broadcast_to(energy, (days * owned, 128)), jnp.broadcast_to(rows, (days * owned, 128))], axis=1
            )
            carry = carry + jnp.sum(both.reshape(days, owned, 256), axis=1)
        return carry

    found = lax.fori_loop(0, chips, statistics, jnp.zeros((days, 256), jnp.float32))
    none = jnp.zeros_like(found)
    stat_out[...] = jnp.where(
        core == 0, jnp.concatenate([found, none], axis=0), jnp.concatenate([none, found], axis=0)
    )
    for o in range(1, peers + 1):
        told(o).start()

    def transform(g, here, cols):
        lhs = rows_ref[g, :, here, :].reshape(-1, lag_count)
        return jnp.dot(lhs, table[:lag_count, cols], preferred_element_type=jnp.float32)

    def add_days(g, here, cols, hilbert):
        size = cols.stop - cols.start
        count = hilbert.shape[0] // all_days
        scale = (day_weight[:, :count] * row_mask[g, :, here, :]).reshape(-1, 1)
        real = scale * rows_ref[g, :, here, cols].reshape(-1, size).astype(jnp.float32)
        imag = scale * hilbert
        inverse = lax.rsqrt(real * real + imag * imag + 0.25)
        for k, term in enumerate((real, real * inverse, imag * inverse)):
            sums[k, :count, cols] = jnp.sum(term.reshape(all_days, count, size), axis=0)

    def encode(piece, rows, o):
        linear, linear_units = codes(sums[0, rows])
        first, first_units = codes(sums[1, rows])
        second, second_units = codes(sums[2, rows])
        words_out[piece, :, :width] = join(first, second)
        words_out[piece, :, width : width + half] = join(linear[:, :half], linear[:, half:])
        pick = lax.broadcasted_iota(jnp.int32, (part, 128), 1)
        words_out[piece, :, width + half :] = jnp.where(
            pick == 0, linear_units, jnp.where(pick == 1, first_units, second_units)
        )
        shipped(piece, o).start()

    def decode(piece, rows):
        units = words_in[piece, :, width + half :].astype(jnp.float32) * (1.0 / (FULL * UNIT))
        left, right = split(words_in[piece, :, width : width + half])
        sums[0, rows, :half] += left.astype(jnp.float32) * units[:, 0:1]
        sums[0, rows, half:] += right.astype(jnp.float32) * units[:, 0:1]
        first, second = split(words_in[piece, :, :width])
        sums[1, rows] += first.astype(jnp.float32) * units[:, 1:2]
        sums[2, rows] += second.astype(jnp.float32) * units[:, 2:3]

    whole, low, high = pl.ds(0, owned), pl.ds(0, part), pl.ds(part, part)

    swapped(order[0]).wait_recv()
    for cols in tiles:
        first_hilbert[:, cols] = transform(order[0], whole, cols)

    for o in range(1, peers + 1):
        told(o).wait_recv()
    stats = stat_out[...]
    for o in range(peers):
        stats = stats + stat_in[o]
    weight = lax.rsqrt(stats[:, :128] / (lag_count * jnp.maximum(stats[:, 128:], 1.0)) + 0.1)
    weight = jnp.where(core == 0, weight, jnp.concatenate([weight[days:], weight[:days]], axis=0))
    for d in range(all_days):
        day_weight[d] = jnp.broadcast_to(weight[d : d + 1, :1], (owned, 1))

    for cols in tiles:
        add_days(order[0], whole, cols, first_hilbert[:, cols])
    encode(0, low, 1)
    encode(1, high, 2)

    def far_block(step, carry):
        o = chips - 1 - step
        swapped(chip ^ o).wait_recv()
        for cols in tiles:
            add_days(chip ^ o, whole, cols, transform(chip ^ o, whole, cols))
        encode(2 * o - 2, low, o)
        encode(2 * o - 1, high, o)
        return carry

    if chips > 4:
        lax.fori_loop(0, chips - 4, far_block, 0)

    def near_half(q, carry):
        o = 1 + q % 2
        g = chip ^ o
        here = pl.ds(pl.multiple_of(((q + q // 2) % 2) * part, part), part)

        @pl.when(q < 2)
        def _():
            swapped(g).wait_recv()

        for cols in tiles:
            add_days(g, here, cols, transform(g, here, cols))

        @pl.when(q >= 2)
        def _():
            shipped(3 - q, o).wait_recv()
            decode(3 - q, low)

        encode(2 + q, low, o)
        return carry

    lax.fori_loop(0, 4, near_half, 0)
    swapped(chip).wait_recv()
    for cols in tiles:
        add_days(chip, whole, cols, transform(chip, whole, cols))

    def arrive(piece, carry):
        turn = piece + jnp.where(piece // 2 == 2, 1, 0)
        shipped(piece, 1).wait_recv()
        decode(piece, pl.ds(pl.multiple_of((turn % 2) * part, part), part))
        return carry

    lax.fori_loop(2, pieces, arrive, 0)
    real, imag = sums[1, :, :lag_count], sums[2, :, :lag_count]
    linear_ref[...] = sums[0, :, :lag_count]
    power_ref[...] = real * real + imag * imag

    mask_copy.wait_send()
    for g in range(chips):
        swapped(g).wait_send()
    for o in range(1, peers + 1):
        told(o).wait_send()
    for piece in range(pieces):
        shipped(piece, 1).wait_send()


def general_sums(correlations, mask):
    days, pairs, lag_count = correlations.shape
    groups = lax.axis_size("day")
    chips = groups // 2
    owned = pairs // groups
    width = padded(lag_count)
    peers = 2 * lax.axis_size("pair") - 1

    strip = jnp.asarray(kernel_strip(lag_count))
    size = width + width // 2 + 128
    pieces = 2 * chips - 2
    out = jax.ShapeDtypeStruct((owned, lag_count), jnp.float32)
    vmem = pl.BlockSpec(memory_space=pltpu.VMEM)
    hbm = pl.BlockSpec(memory_space=pl.ANY)
    dma = pltpu.SemaphoreType.DMA
    return pl.pallas_call(
        functools.partial(stack_kernel, lag_count),
        in_specs=[hbm, vmem, hbm],
        out_specs=(vmem, vmem),
        out_shape=(out, out),
        scratch_shapes=[
            pltpu.VMEM((chips, 2 * days, owned, lag_count), jnp.bfloat16),
            pltpu.VMEM((chips, days, owned, lag_count), jnp.bfloat16),
            pltpu.VMEM(strip.shape, jnp.bfloat16),
            pltpu.VMEM((width, width), jnp.bfloat16),
            pltpu.VMEM((3, owned, width), jnp.float32),
            pltpu.VMEM((2 * days * owned, width), jnp.float32),
            pltpu.VMEM((days, pairs), jnp.int32),
            pltpu.VMEM((pairs, 2 * days), jnp.float32),
            pltpu.VMEM((chips, 2 * days, owned, 1), jnp.float32),
            pltpu.VMEM((2 * days, owned, 1), jnp.float32),
            pltpu.VMEM((2 * days, 256), jnp.float32),
            pltpu.VMEM((peers, 2 * days, 256), jnp.float32),
            pltpu.VMEM((pieces, owned // 2, size), jnp.int32),
            pltpu.VMEM((pieces, owned // 2, size), jnp.int32),
            dma((chips,)), dma((chips,)), dma, dma((chips,)), dma((chips,)), dma, dma,
            dma((peers,)), dma((peers,)), dma((pieces,)), dma((pieces,)),
        ],
        compiler_params=pltpu.CompilerParams(
            vmem_limit_bytes=46 * 2**20, collective_id=0, has_side_effects=True
        ),
        name="stack",
    )(correlations.reshape(days, groups, owned, lag_count), mask, strip)


LANES = 128
CHUNK = 512
HALF = CHUNK // 2
ROWS = HALF // 2
WORDS = ROWS + ROWS // 2
PACK = WORDS + 8


def block_strip(lag_count):
    f32 = np.float32
    offset = np.arange(lag_count, dtype=np.int32)
    offset = np.where(offset > lag_count // 2, offset - lag_count, offset)
    angle = f32(np.pi) * offset.astype(f32) / f32(lag_count)
    parity = f32(1) - f32(2) * (offset % 2).astype(f32)
    sine = np.where(offset == 0, f32(1), np.sin(angle)).astype(f32)
    kernel = np.where(offset == 0, f32(0), (np.cos(angle) - parity) / (f32(lag_count) * sine))
    width = chunked(lag_count)
    index = np.arange(TILE)[:, None] - np.arange(2 * width - TILE)[None, :] + (width - TILE)
    return kernel.astype(f32)[index % lag_count].astype(jnp.bfloat16)


def chunked(lag_count):
    return -(-lag_count // CHUNK) * CHUNK


def sorting_matrix(rows):
    lags = TILE // rows
    out = np.arange(TILE)
    source = (out % lags) * rows + out // lags
    return (source[:, None] == np.arange(TILE)[None, :]).astype(jnp.bfloat16)


def fast_kernel(
    lag_count, x_hbm, mask_ref, strip, sorter, linear_ref, power_ref,
    raw, own, theirs, first_h, second_h, sums, scale, bias, mask_in, stat_out, stat_in,
    partial_out, partial_in, final_out, final_in, own_out, total,
    load_sem, swap_send, swap_recv, late_send, late_recv, mask_send, mask_recv, stat_send, stat_recv,
    partial_send, partial_recv, final_send, final_recv, own_send, own_recv,
):
    f32 = jnp.float32
    width = raw.shape[0]
    planes = raw.shape[1]
    loads = width // TILE
    steps = width // CHUNK
    peers = stat_in.shape[0]
    days = mask_ref.shape[0]
    tiles = mask_ref.shape[1] // LANES
    lags = TILE // planes
    me, plane = lax.axis_index("day"), lax.axis_index("pair")
    chip, core = me // 2, me % 2
    partner = {"day": me ^ 1, "pair": plane}

    def near(o, c):
        return {"day": 2 * (chip ^ o) + c, "pair": plane}

    def peer(o):
        rank = (2 * plane + core + o) % (peers + 1)
        return {"day": 2 * chip + rank % 2, "pair": rank // 2}

    def loaded(j, count=TILE):
        rows = pl.ds(j * TILE, count)
        return pltpu.make_async_copy(x_hbm.at[rows], raw.at[rows], load_sem.at[j])

    def remote(source, target, send, recv, device):
        return pltpu.make_async_remote_copy(
            source, target, send, recv, device_id=device, device_id_type=MESH
        )

    def mine(slot):
        return 2 * (1 - core) + 1 - slot

    def swapped(j):
        rows = pl.ds(pl.multiple_of(j * TILE, TILE), TILE)
        return remote(
            own.at[2 * core + 1, :, rows], theirs.at[0, :, rows], swap_send.at[j], swap_recv.at[j], partner
        )

    def swapped_late():
        return remote(own.at[2 * core], theirs.at[1], late_send, late_recv, partner)

    def told(o):
        return remote(stat_out, stat_in.at[o - 1], stat_send.at[o - 1], stat_recv.at[o - 1], peer(o))

    def relayed(k, half):
        return remote(
            partial_out.at[k, half], partial_in.at[k], partial_send.at[k, half], partial_recv.at[k],
            near(1 + half, half),
        )

    def finished(k, half, c):
        return remote(
            final_out.at[k, half, c], final_in.at[1 - core, k, half], final_send.at[k, half, c],
            final_recv.at[1 - core, k, half], near(2 - core, c),
        )

    def handed(k, half):
        return remote(own_out.at[k, half], total.at[k, half], own_send.at[k, half], own_recv.at[k, half], partner)

    last = loads - 1
    for j in range(last):
        loaded(j).start()
    loaded(last, lag_count - last * TILE).start()
    barrier = pltpu.get_barrier_semaphore()
    for o in range(1, peers + 1):
        pl.semaphore_signal(barrier, inc=1, device_id=peer(o), device_id_type=MESH)
    for o in (1, 2):
        for c in (0, 1):
            pl.semaphore_signal(barrier, inc=1, device_id=near(o, c), device_id_type=MESH)
    raw[lag_count:] = jnp.zeros((width - lag_count, planes, LANES), raw.dtype)
    pl.semaphore_wait(barrier, peers + 4)
    mask_copy = remote(mask_ref, mask_in, mask_send, mask_recv, partner)
    mask_copy.start()

    def sort(j, energy):
        energy = [energy[i] for i in range(planes)]
        for g in range(TILE // (2 * lags)):
            at = pl.multiple_of(j * TILE + g * 2 * lags, 2 * lags)
            pair = [raw[pl.ds(at + h * lags, lags)].reshape(TILE, LANES) for h in (0, 1)]
            out = jnp.dot(sorter[...], jnp.concatenate(pair, axis=1), preferred_element_type=f32)
            for t in range(tiles):
                for d in range(days):
                    i = t * days + d
                    lane = (d % 2) * LANES
                    for h in (0, 1):
                        value = out[i * lags : (i + 1) * lags, h * LANES : (h + 1) * LANES]
                        energy[i] = energy[i] + jnp.sum((value * value).reshape(-1, 8, LANES), axis=0)
                        own[chip ^ t, d // 2, pl.ds(at + h * lags, lags), lane : lane + LANES] = value.astype(own.dtype)
        return jnp.stack(energy)

    def sort_load(j, energy):
        loaded(j).wait()
        energy = sort(j, energy)
        swapped(j).start()
        return energy

    energy = lax.fori_loop(0, last, sort_load, jnp.zeros((planes, 8, LANES), f32))
    loaded(last, lag_count - last * TILE).wait()
    energy = sort(last, energy)
    swapped(last).start()
    swapped_late().start()

    found, used = [], []
    for d in range(days):
        rows = [mask_ref[d : d + 1, t * LANES : (t + 1) * LANES].astype(f32) for t in range(tiles)]
        one = sum(jnp.sum(energy[t * days + d], axis=0, keepdims=True) * rows[t] for t in range(tiles))
        found.append(one)
        used.append(sum(rows))
    stat_out[...] = jnp.concatenate(found + used, axis=0)
    for o in range(1, peers + 1):
        told(o).start()

    def operand(slot, dp):
        return own[mine(slot), dp] if dp < days // 2 else theirs[slot, dp - days // 2]

    def transform(slot, k, dps, target):
        for dp in dps:
            rhs = operand(slot, dp)
            for part in range(CHUNK // TILE):
                start = pl.multiple_of(width - TILE - (k * (CHUNK // TILE) + part) * TILE, TILE)
                target[part * TILE : (part + 1) * TILE, dp * TILE : (dp + 1) * TILE] = jnp.dot(
                    strip[:, pl.ds(start, width)], rhs, preferred_element_type=f32
                )

    def add_days(slot, k, first, count, source):
        size = 32
        for row in range(first, first + count, size):
            at = pl.multiple_of(k * CHUNK + row, size)
            lin = one = two = jnp.zeros((size // 8, 8, LANES), f32)
            for e in range(2 * days):
                dp, lane = e // 2, (e % 2) * LANES
                if e < days:
                    x = own[mine(slot), dp, pl.ds(at, size), lane : lane + LANES]
                else:
                    x = theirs[slot, dp - days // 2, pl.ds(at, size), lane : lane + LANES]
                x = x.astype(f32).reshape(size // 8, 8, LANES)
                h = source[row : row + size, e * LANES : (e + 1) * LANES].reshape(size // 8, 8, LANES)
                r = lax.rsqrt(x * x + h * h + bias[slot, e][None])
                lin = lin + x * scale[slot, e][None]
                one = one + x * r
                two = two + h * r
            for v, value in enumerate((lin, one, two)):
                sums[slot, v, row : row + size] = value.reshape(size, LANES)

    low_lane = lax.broadcasted_iota(jnp.int32, (ROWS, LANES), 1) < LANES // 2

    def split(slot, half, v, c):
        a = sums[slot, v, half * HALF : half * HALF + ROWS]
        b = sums[slot, v, half * HALF + ROWS : (half + 1) * HALF]
        if c == 0:
            return jnp.where(low_lane, a, pltpu.roll(b, LANES // 2, 1))
        return jnp.where(low_lane, pltpu.roll(a, LANES // 2, 1), b)

    def encode(target, values):
        coded, units = [], []
        for value in values:
            top = jnp.max(jnp.abs(value), axis=0, keepdims=True)
            unit = (top * UNIT).astype(jnp.int32) + 1
            step = FULL * UNIT / unit.astype(f32)
            coded.append((value * step + 32768.5).astype(jnp.int32))
            units.append(unit)
        lin, one, two = coded
        target[:ROWS] = one * 65536 + two
        target[ROWS:WORDS] = lin[: ROWS // 2] * 65536 + lin[ROWS // 2 :]
        pick = lax.broadcasted_iota(jnp.int32, (8, LANES), 0)
        target[WORDS:] = jnp.where(pick == 0, units[0], jnp.where(pick == 1, units[1], units[2]))

    def decode(source):
        units = source[WORDS:].astype(f32) * (1.0 / (FULL * UNIT))

        def value(code, v):
            return (code.astype(f32) - 32768.0) * units[v : v + 1]

        def pieces(word):
            return lax.shift_right_logical(word, jnp.full_like(word, 16)), word & 65535

        one, two = pieces(source[:ROWS])
        top, bottom = pieces(source[ROWS:WORDS])
        return (jnp.concatenate([value(top, 0), value(bottom, 0)], axis=0), value(one, 1), value(two, 2))

    def send_direct(slot, k, half):
        for c in (0, 1):
            encode(final_out.at[k, half, c], [split(slot, half, v, c) for v in range(3)])
            finished(k, half, c).start()

    def send_relayed(slot, k, half):
        relayed(k, half).wait_recv()
        for c in (0, 1):
            far = decode(partial_in.at[k, c])
            encode(final_out.at[k, half, c], [split(slot, half, v, c) + far[v] for v in range(3)])
            finished(k, half, c).start()

    def finish_first(k):
        @pl.when(core == 0)
        def _():
            for half in (0, 1):
                for c in (0, 1):
                    encode(partial_out.at[k, half, c], [split(0, half, v, c) for v in range(3)])
                relayed(k, half).start()

        @pl.when(core == 1)
        def _():
            send_direct(0, k, 0)

    def finish_second(k):
        @pl.when(core == 0)
        def _():
            send_direct(1, k, 1)
            send_relayed(1, k, 0)

        @pl.when(core == 1)
        def _():
            for half in (0, 1):
                for v in range(3):
                    own_out[k, half, v] = split(1, half, v, 0)
                    total[k, half, v] = split(1, half, v, 1)
                handed(k, half).start()
            send_relayed(0, k, 1)

    for j in range(loads):
        swapped(j).wait_recv()
    dps = range(days)
    transform(0, 0, dps, first_h)

    mask_copy.wait_recv()
    for o in range(1, peers + 1):
        told(o).wait_recv()
    ours, other = stat_out[...], jnp.zeros_like(stat_out)
    for o in range(1, peers + 1):
        if o % 2:
            other = other + stat_in[o - 1]
        else:
            ours = ours + stat_in[o - 1]
    for which, stats in enumerate((ours, other)):
        row = jnp.sum(stats, axis=1, keepdims=True)
        power = row[:days] / (lag_count * jnp.maximum(row[days:], 1.0)) + 0.1
        weight = lax.rsqrt(power)
        for slot in (0, 1):
            at = pl.multiple_of((chip ^ mine(slot)) * LANES, LANES)
            usable = (mask_in if which else mask_ref)[:, pl.ds(at, LANES)].astype(f32)
            by_day = weight * usable
            offset = jnp.where(usable > 0.0, 0.25 * power, jnp.inf)
            for d in range(days):
                scale[slot, which * days + d] = jnp.broadcast_to(by_day[d : d + 1], (8, LANES))
                bias[slot, which * days + d] = jnp.broadcast_to(offset[d : d + 1], (8, LANES))
    swapped_late().wait_recv()

    def step(k, carry):
        for q in range(2):
            transform(1, k, (q,), second_h)
            add_days(0, k, q * HALF, HALF, first_h)
        finish_first(k)
        for q in range(2, 4):
            transform(1, k, (q,), second_h)
        ahead = jnp.minimum(k + 1, steps - 1)
        for q in range(2):
            transform(0, ahead, (q,), first_h)
            add_days(1, k, q * HALF, HALF, second_h)
        finish_second(k)
        for q in range(2, 4):
            transform(0, ahead, (q,), first_h)
        return carry

    lax.fori_loop(0, steps, step, 0)

    def gather(k, carry):
        for half in (0, 1):
            @pl.when(core == 0)
            def _():
                handed(k, half).wait_recv()

            for s in (0, 1):
                remote(
                    final_out.at[k, half, 0], final_in.at[s, k, half], final_send.at[k, half, 0],
                    final_recv.at[s, k, half], partner,
                ).wait_recv()
                far = decode(final_in.at[s, k, half])
                for v in range(3):
                    total[k, half, v] += far[v]
        return carry

    lax.fori_loop(0, steps, gather, 0)
    for k in range(steps):
        for half in (0, 1):
            lin, one, two = (total[k, half, v] for v in range(3))
            for ref, value in ((linear_ref, lin), (power_ref, one * one + two * two)):
                turned = value.T
                for part in (0, 1):
                    start = k * CHUNK + half * HALF + part * ROWS
                    stop = min(start + ROWS, lag_count)
                    if stop > start:
                        rows = turned[part * LANES // 2 : (part + 1) * LANES // 2]
                        ref[:, start:stop] = rows[:, : stop - start]

    mask_copy.wait_send()
    swapped_late().wait_send()
    for j in range(loads):
        swapped(j).wait_send()
    for o in range(1, peers + 1):
        told(o).wait_send()
    for k in range(steps):
        for half in (0, 1):
            for c in (0, 1):
                finished(k, half, c).wait_send()

            @pl.when(core == 0)
            def _():
                relayed(k, half).wait_send()

            @pl.when(core == 1)
            def _():
                handed(k, half).wait_send()


def fast_sums(correlations, mask):
    days, pairs, lag_count = correlations.shape
    owned = pairs // lax.axis_size("day")
    peers = 2 * lax.axis_size("pair") - 1
    tiles = pairs // LANES
    planes = tiles * days
    width = chunked(lag_count)
    steps, loads = width // CHUNK, width // TILE
    by_lag = correlations.transpose(2, 0, 1).reshape(lag_count, days, tiles, LANES)
    by_lag = by_lag.transpose(0, 2, 1, 3).reshape(lag_count, planes, LANES)
    out = jax.ShapeDtypeStruct((owned, lag_count), jnp.float32)
    vmem = pl.BlockSpec(memory_space=pltpu.VMEM)
    hbm = pl.BlockSpec(memory_space=pl.ANY)
    dma = pltpu.SemaphoreType.DMA
    bf16, f32, i32 = jnp.bfloat16, jnp.float32, jnp.int32
    return pl.pallas_call(
        functools.partial(fast_kernel, lag_count),
        in_specs=[hbm, vmem, vmem, vmem],
        out_specs=(vmem, vmem),
        out_shape=(out, out),
        scratch_shapes=[
            pltpu.VMEM((width, planes, LANES), bf16),
            pltpu.VMEM((tiles, days // 2, width, TILE), bf16),
            pltpu.VMEM((2, days // 2, width, TILE), bf16),
            pltpu.VMEM((CHUNK, 2 * days * LANES), f32),
            pltpu.VMEM((CHUNK, 2 * days * LANES), f32),
            pltpu.VMEM((2, 3, CHUNK, LANES), f32),
            pltpu.VMEM((2, 2 * days, 8, LANES), f32),
            pltpu.VMEM((2, 2 * days, 8, LANES), f32),
            pltpu.VMEM(mask.shape, i32),
            pltpu.VMEM((2 * days, LANES), f32),
            pltpu.VMEM((peers, 2 * days, LANES), f32),
            pltpu.VMEM((steps, 2, 2, PACK, LANES), i32),
            pltpu.VMEM((steps, 2, PACK, LANES), i32),
            pltpu.VMEM((steps, 2, 2, PACK, LANES), i32),
            pltpu.VMEM((2, steps, 2, PACK, LANES), i32),
            pltpu.VMEM((steps, 2, 3, ROWS, LANES), f32),
            pltpu.VMEM((steps, 2, 3, ROWS, LANES), f32),
            dma((loads,)), dma((loads,)), dma((loads,)), dma, dma, dma, dma, dma((peers,)), dma((peers,)),
            dma((steps, 2)), dma((steps,)), dma((steps, 2, 2)), dma((2, steps, 2)), dma((steps, 2)), dma((steps, 2)),
        ],
        compiler_params=pltpu.CompilerParams(
            vmem_limit_bytes=58 * 2**20, collective_id=0, has_side_effects=True
        ),
        name="stack",
    )(by_lag, mask, jnp.asarray(block_strip(lag_count)), jnp.asarray(sorting_matrix(planes)))


def shards(correlations, mask, counts):
    days, pairs, lag_count = correlations.shape
    groups = lax.axis_size("day")
    fits = groups == 8 and days == 4 and pairs == groups // 2 * LANES
    linear_sum, power = (fast_sums if fits else general_sums)(correlations, mask)
    inverse = (1.0 / jnp.maximum(counts.astype(jnp.float32), 1.0))[:, None]
    linear = linear_sum * inverse
    return (linear * (power * (inverse * inverse)), linear)


def solution(mesh):
    placed = (P("day", "pair", None), P("day", "pair"), P(("pair", "day")))
    return jax.shard_map(
        shards,
        mesh=mesh,
        in_specs=placed,
        out_specs=(P(("pair", "day"), None), P(("pair", "day"), None)),
        check_vma=False,
    )
```

```python
import functools

import jax
import jax.numpy as jnp
import numpy as np
from jax import lax
from jax.experimental import pallas as pl
from jax.experimental.pallas import tpu as pltpu
from jax.sharding import PartitionSpec as P

TILE = 256
MESH = pl.DeviceIdType.MESH
FULL = 32767.0
UNIT = 2.0**20


def padded(lag_count):
    return -(-lag_count // TILE) * TILE


def kernel_strip(lag_count):
    f32 = np.float32
    offset = np.arange(lag_count, dtype=np.int32)
    offset = np.where(offset > lag_count // 2, offset - lag_count, offset)
    angle = f32(np.pi) * offset.astype(f32) / f32(lag_count)
    parity = f32(1) - f32(2) * (offset % 2).astype(f32)
    sine = np.where(offset == 0, f32(1), np.sin(angle)).astype(f32)
    kernel = np.where(offset == 0, f32(0), (np.cos(angle) - parity) / (f32(lag_count) * sine))
    width = padded(lag_count)
    index = np.arange(2 * width - TILE)[None, :] - np.arange(TILE)[:, None] - (width - TILE)
    return kernel.astype(f32)[index % lag_count].astype(jnp.bfloat16)


def codes(values):
    top = jnp.max(jnp.abs(values), axis=1, keepdims=True)
    units = (top * UNIT).astype(jnp.int32) + 1
    step = FULL * UNIT / units.astype(jnp.float32)
    return jnp.round(values * step).astype(jnp.int32), units


def join(high, low):
    return high * 65536 + (low & 65535)


def split(word):
    low = ((word & 65535) ^ 32768) - 32768
    return word >> 16, low


def stack_kernel(
    lag_count, x_hbm, mask_ref, strip_hbm, linear_ref, power_ref,
    rows_ref, stage, strip, table, sums, first_hilbert, mask_in, mask_turned, row_mask, day_weight,
    stat_out, stat_in, words_out, words_in,
    load_sem, stage_sem, strip_sem, swap_send, swap_recv, mask_send, mask_recv,
    stat_send, stat_recv, word_send, word_recv,
):
    width = table.shape[1]
    half = width // 2
    chips, all_days, owned, _ = rows_ref.shape
    days = all_days // 2
    total = all_days * owned
    part = owned // 2
    pieces = words_out.shape[0]
    peers = stat_in.shape[0]
    me, plane = lax.axis_index("day"), lax.axis_index("pair")
    chip, core = me // 2, me % 2
    partner = {"day": me ^ 1, "pair": plane}
    last = width - TILE
    tiles = [slice(j * TILE, min((j + 1) * TILE, lag_count)) for j in range(width // TILE)]

    def mine(g):
        return pltpu.make_async_copy(x_hbm.at[:, 2 * g + core], rows_ref.at[g, pl.ds(0, days)], load_sem.at[g])

    def staged(g):
        return pltpu.make_async_copy(x_hbm.at[:, 2 * g + 1 - core], stage.at[g], stage_sem.at[g])

    def swapped(g):
        return pltpu.make_async_remote_copy(
            stage.at[g], rows_ref.at[g, pl.ds(days, days)], swap_send.at[g], swap_recv.at[g],
            device_id=partner, device_id_type=MESH,
        )

    def peer(o):
        rank = (2 * plane + core + o) % (peers + 1)
        return {"day": 2 * chip + rank % 2, "pair": rank // 2}

    def told(o):
        return pltpu.make_async_remote_copy(
            stat_out, stat_in.at[o - 1], stat_send.at[o - 1], stat_recv.at[o - 1],
            device_id=peer(o), device_id_type=MESH,
        )

    def owner(o):
        return {"day": 2 * (chip ^ o) + core, "pair": plane}

    def shipped(piece, o):
        return pltpu.make_async_remote_copy(
            words_out.at[piece], words_in.at[piece], word_send.at[piece], word_recv.at[piece],
            device_id=owner(o), device_id_type=MESH,
        )

    far = range(chips - 1, 3, -1)
    order = [chip ^ o for o in (3, *far, 1, 2, 0)]
    strip_copy = pltpu.make_async_copy(strip_hbm, strip, strip_sem)
    strip_copy.start()
    for g in order:
        staged(g).start()
        mine(g).start()

    barrier = pltpu.get_barrier_semaphore()
    for o in range(1, peers + 1):
        pl.semaphore_signal(barrier, inc=1, device_id=peer(o), device_id_type=MESH)
    for o in range(1, chips):
        pl.semaphore_signal(barrier, inc=1, device_id=owner(o), device_id_type=MESH)
    strip_copy.wait()
    for i in range(width // TILE):
        start = width - TILE - i * TILE
        table[pl.ds(i * TILE, TILE), :] = strip[:, start : start + width]
    sums[:, :, last:] = jnp.zeros((3, owned, TILE), jnp.float32)
    pl.semaphore_wait(barrier, peers + chips - 1)

    mask_copy = pltpu.make_async_remote_copy(
        mask_ref, mask_in, mask_send, mask_recv, device_id=partner, device_id_type=MESH
    )
    mask_copy.start()
    for g in order:
        staged(g).wait()
        swapped(g).start()
    mask_copy.wait_recv()
    both_masks = jnp.concatenate([mask_ref[...], mask_in[...]], axis=0).astype(jnp.float32)
    mask_turned[...] = both_masks.T

    def mask_rows(block, count):
        rows = mask_turned[pl.ds(pl.multiple_of(block * owned, owned), owned), :]
        return jnp.concatenate([rows[:, d : d + 1] for d in range(count)], axis=0)

    def statistics(step, carry):
        g = chip ^ (chips - 1 - step)
        mine(g).wait()
        of_pairs = mask_rows(2 * g + core, all_days)
        row_mask[g] = of_pairs.reshape(all_days, owned, 1)
        for x_ref, rows in ((rows_ref.at[g, pl.ds(0, days)], of_pairs[: days * owned]),
                            (stage.at[g], mask_rows(2 * g + 1 - core, days))):
            x = x_ref[...].reshape(days * owned, lag_count).astype(jnp.float32)
            energy = jnp.sum(x * x, axis=1, keepdims=True) * rows
            both = jnp.concatenate(
                [jnp.broadcast_to(energy, (days * owned, 128)), jnp.broadcast_to(rows, (days * owned, 128))], axis=1
            )
            carry = carry + jnp.sum(both.reshape(days, owned, 256), axis=1)
        return carry

    found = lax.fori_loop(0, chips, statistics, jnp.zeros((days, 256), jnp.float32))
    none = jnp.zeros_like(found)
    stat_out[...] = jnp.where(
        core == 0, jnp.concatenate([found, none], axis=0), jnp.concatenate([none, found], axis=0)
    )
    for o in range(1, peers + 1):
        told(o).start()

    def transform(g, here, cols):
        lhs = rows_ref[g, :, here, :].reshape(-1, lag_count)
        return jnp.dot(lhs, table[:lag_count, cols], preferred_element_type=jnp.float32)

    def add_days(g, here, cols, hilbert):
        size = cols.stop - cols.start
        count = hilbert.shape[0] // all_days
        scale = (day_weight[:, :count] * row_mask[g, :, here, :]).reshape(-1, 1)
        real = scale * rows_ref[g, :, here, cols].reshape(-1, size).astype(jnp.float32)
        imag = scale * hilbert
        inverse = lax.rsqrt(real * real + imag * imag + 0.25)
        for k, term in enumerate((real, real * inverse, imag * inverse)):
            sums[k, :count, cols] = jnp.sum(term.reshape(all_days, count, size), axis=0)

    def encode(piece, rows, o):
        linear, linear_units = codes(sums[0, rows])
        first, first_units = codes(sums[1, rows])
        second, second_units = codes(sums[2, rows])
        words_out[piece, :, :width] = join(first, second)
        words_out[piece, :, width : width + half] = join(linear[:, :half], linear[:, half:])
        pick = lax.broadcasted_iota(jnp.int32, (part, 128), 1)
        words_out[piece, :, width + half :] = jnp.where(
            pick == 0, linear_units, jnp.where(pick == 1, first_units, second_units)
        )
        shipped(piece, o).start()

    def decode(piece, rows):
        units = words_in[piece, :, width + half :].astype(jnp.float32) * (1.0 / (FULL * UNIT))
        left, right = split(words_in[piece, :, width : width + half])
        sums[0, rows, :half] += left.astype(jnp.float32) * units[:, 0:1]
        sums[0, rows, half:] += right.astype(jnp.float32) * units[:, 0:1]
        first, second = split(words_in[piece, :, :width])
        sums[1, rows] += first.astype(jnp.float32) * units[:, 1:2]
        sums[2, rows] += second.astype(jnp.float32) * units[:, 2:3]

    whole, low, high = pl.ds(0, owned), pl.ds(0, part), pl.ds(part, part)

    swapped(order[0]).wait_recv()
    for cols in tiles:
        first_hilbert[:, cols] = transform(order[0], whole, cols)

    for o in range(1, peers + 1):
        told(o).wait_recv()
    stats = stat_out[...]
    for o in range(peers):
        stats = stats + stat_in[o]
    weight = lax.rsqrt(stats[:, :128] / (lag_count * jnp.maximum(stats[:, 128:], 1.0)) + 0.1)
    weight = jnp.where(core == 0, weight, jnp.concatenate([weight[days:], weight[:days]], axis=0))
    for d in range(all_days):
        day_weight[d] = jnp.broadcast_to(weight[d : d + 1, :1], (owned, 1))

    for cols in tiles:
        add_days(order[0], whole, cols, first_hilbert[:, cols])
    encode(0, low, 1)
    encode(1, high, 2)

    def far_block(step, carry):
        o = chips - 1 - step
        swapped(chip ^ o).wait_recv()
        for cols in tiles:
            add_days(chip ^ o, whole, cols, transform(chip ^ o, whole, cols))
        encode(2 * o - 2, low, o)
        encode(2 * o - 1, high, o)
        return carry

    if chips > 4:
        lax.fori_loop(0, chips - 4, far_block, 0)

    def near_half(q, carry):
        o = 1 + q % 2
        g = chip ^ o
        here = pl.ds(pl.multiple_of(((q + q // 2) % 2) * part, part), part)

        @pl.when(q < 2)
        def _():
            swapped(g).wait_recv()

        for cols in tiles:
            add_days(g, here, cols, transform(g, here, cols))

        @pl.when(q >= 2)
        def _():
            shipped(3 - q, o).wait_recv()
            decode(3 - q, low)

        encode(2 + q, low, o)
        return carry

    lax.fori_loop(0, 4, near_half, 0)
    swapped(chip).wait_recv()
    for cols in tiles:
        add_days(chip, whole, cols, transform(chip, whole, cols))

    def arrive(piece, carry):
        turn = piece + jnp.where(piece // 2 == 2, 1, 0)
        shipped(piece, 1).wait_recv()
        decode(piece, pl.ds(pl.multiple_of((turn % 2) * part, part), part))
        return carry

    lax.fori_loop(2, pieces, arrive, 0)
    real, imag = sums[1, :, :lag_count], sums[2, :, :lag_count]
    linear_ref[...] = sums[0, :, :lag_count]
    power_ref[...] = real * real + imag * imag

    mask_copy.wait_send()
    for g in range(chips):
        swapped(g).wait_send()
    for o in range(1, peers + 1):
        told(o).wait_send()
    for piece in range(pieces):
        shipped(piece, 1).wait_send()


def general_sums(correlations, mask):
    days, pairs, lag_count = correlations.shape
    groups = lax.axis_size("day")
    chips = groups // 2
    owned = pairs // groups
    width = padded(lag_count)
    peers = 2 * lax.axis_size("pair") - 1

    strip = jnp.asarray(kernel_strip(lag_count))
    size = width + width // 2 + 128
    pieces = 2 * chips - 2
    out = jax.ShapeDtypeStruct((owned, lag_count), jnp.float32)
    vmem = pl.BlockSpec(memory_space=pltpu.VMEM)
    hbm = pl.BlockSpec(memory_space=pl.ANY)
    dma = pltpu.SemaphoreType.DMA
    return pl.pallas_call(
        functools.partial(stack_kernel, lag_count),
        in_specs=[hbm, vmem, hbm],
        out_specs=(vmem, vmem),
        out_shape=(out, out),
        scratch_shapes=[
            pltpu.VMEM((chips, 2 * days, owned, lag_count), jnp.bfloat16),
            pltpu.VMEM((chips, days, owned, lag_count), jnp.bfloat16),
            pltpu.VMEM(strip.shape, jnp.bfloat16),
            pltpu.VMEM((width, width), jnp.bfloat16),
            pltpu.VMEM((3, owned, width), jnp.float32),
            pltpu.VMEM((2 * days * owned, width), jnp.float32),
            pltpu.VMEM((days, pairs), jnp.int32),
            pltpu.VMEM((pairs, 2 * days), jnp.float32),
            pltpu.VMEM((chips, 2 * days, owned, 1), jnp.float32),
            pltpu.VMEM((2 * days, owned, 1), jnp.float32),
            pltpu.VMEM((2 * days, 256), jnp.float32),
            pltpu.VMEM((peers, 2 * days, 256), jnp.float32),
            pltpu.VMEM((pieces, owned // 2, size), jnp.int32),
            pltpu.VMEM((pieces, owned // 2, size), jnp.int32),
            dma((chips,)), dma((chips,)), dma, dma((chips,)), dma((chips,)), dma, dma,
            dma((peers,)), dma((peers,)), dma((pieces,)), dma((pieces,)),
        ],
        compiler_params=pltpu.CompilerParams(
            vmem_limit_bytes=46 * 2**20, collective_id=0, has_side_effects=True
        ),
        name="stack",
    )(correlations.reshape(days, groups, owned, lag_count), mask, strip)


LANES = 128
CHUNK = 512
HALF = CHUNK // 2
ROWS = HALF // 2
WORDS = ROWS + ROWS // 2
PACK = WORDS + 8
SENT = WORDS + 3


def block_strip(lag_count):
    f32 = np.float32
    offset = np.arange(lag_count, dtype=np.int32)
    offset = np.where(offset > lag_count // 2, offset - lag_count, offset)
    angle = f32(np.pi) * offset.astype(f32) / f32(lag_count)
    parity = f32(1) - f32(2) * (offset % 2).astype(f32)
    sine = np.where(offset == 0, f32(1), np.sin(angle)).astype(f32)
    kernel = np.where(offset == 0, f32(0), (np.cos(angle) - parity) / (f32(lag_count) * sine))
    width = chunked(lag_count)
    index = np.arange(TILE)[:, None] - np.arange(2 * width - TILE)[None, :] + (width - TILE)
    return kernel.astype(f32)[index % lag_count].astype(jnp.bfloat16)


def chunked(lag_count):
    return -(-lag_count // CHUNK) * CHUNK


def sorting_matrix(rows):
    lags = TILE // rows
    out = np.arange(TILE)
    source = (out % lags) * rows + out // lags
    return (source[:, None] == np.arange(TILE)[None, :]).astype(jnp.bfloat16)


def fast_kernel(
    lag_count, x_hbm, mask_ref, counts_ref, strip_hbm, sorter, weighted_ref, linear_ref,
    raw, own, theirs, strip, even_h, odd_h, sums, scale, bias, mask_in, stat_out, stat_in,
    coded, parts, partial_in, relay_out, final_in, total, inverse,
    load_sem, strip_sem, swap_send, swap_recv, late_send, late_recv, mask_send, mask_recv, stat_send, stat_recv,
    partial_send, partial_recv, final_send, final_recv, own_send, own_recv,
):
    f32 = jnp.float32
    width = raw.shape[0]
    planes = raw.shape[1]
    loads = width // TILE
    chunks = width // CHUNK
    steps = 2 * chunks
    peers = stat_in.shape[0]
    days = mask_ref.shape[0]
    tiles = mask_ref.shape[1] // LANES
    lags = TILE // planes
    me, plane = lax.axis_index("day"), lax.axis_index("pair")
    chip, core = me // 2, me % 2
    partner = {"day": me ^ 1, "pair": plane}

    def order(s):
        inner = (s + 1) % 2
        slot = jnp.where(s == 0, 0, jnp.where(s == steps - 1, 1, inner))
        k = jnp.where(s == 0, 0, jnp.where(s == steps - 1, chunks - 1, jnp.where(inner == 0, (s + 1) // 2, (s - 2) // 2)))
        return jnp.where(core == 0, slot, s // chunks), jnp.where(core == 0, k, s % chunks)

    def near_step(k):
        return jnp.where(core == 0, jnp.where(k == chunks - 1, steps - 1, 2 * k + 2), k)

    def near(o, c):
        return {"day": 2 * (chip ^ o) + c, "pair": plane}

    def peer(o):
        rank = (2 * plane + core + o) % (peers + 1)
        return {"day": 2 * chip + rank % 2, "pair": rank // 2}

    def loaded(j, count=TILE):
        rows = pl.ds(j * TILE, count)
        return pltpu.make_async_copy(x_hbm.at[rows], raw.at[rows], load_sem.at[j])

    def remote(source, target, send, recv, device):
        return pltpu.make_async_remote_copy(
            source, target, send, recv, device_id=device, device_id_type=MESH
        )

    def mine(slot):
        return 2 * (1 - core) + 1 - slot

    def swapped(j):
        rows = pl.ds(pl.multiple_of(j * TILE, TILE), TILE)
        return remote(
            own.at[2 * core + 1, :, rows], theirs.at[0, :, rows], swap_send.at[j], swap_recv.at[j], partner
        )

    def swapped_late():
        return remote(own.at[2 * core], theirs.at[1], late_send, late_recv, partner)

    def told(o):
        return remote(stat_out, stat_in.at[o - 1], stat_send.at[o - 1], stat_recv.at[o - 1], peer(o))

    sent = pl.ds(0, SENT)

    def relayed(s, k, half):
        return remote(
            coded.at[s, half, :, sent], partial_in.at[k, :, sent], partial_send.at[k, half], partial_recv.at[k],
            near(1 + half, half),
        )

    def finished(source, k, half, c):
        return remote(
            source.at[sent], final_in.at[1 - core, k, half, sent], final_send.at[k, half, c],
            final_recv.at[1 - core, k, half], near(2 - core, c),
        )

    def handed(s, k, half):
        return remote(
            parts.at[s, half, 0], total.at[k, half], own_send.at[k, half], own_recv.at[k, half], partner
        )

    last = loads - 1
    for j in range(last):
        loaded(j).start()
    loaded(last, lag_count - last * TILE).start()
    strip_copy = pltpu.make_async_copy(strip_hbm, strip, strip_sem)
    strip_copy.start()
    barrier = pltpu.get_barrier_semaphore()
    for o in range(1, peers + 1):
        pl.semaphore_signal(barrier, inc=1, device_id=peer(o), device_id_type=MESH)
    for o in (1, 2):
        for c in (0, 1):
            pl.semaphore_signal(barrier, inc=1, device_id=near(o, c), device_id_type=MESH)
    raw[lag_count:] = jnp.zeros((width - lag_count, planes, LANES), raw.dtype)
    pl.semaphore_wait(barrier, peers + 4)
    mask_copy = remote(mask_ref, mask_in, mask_send, mask_recv, partner)
    mask_copy.start()

    def sort(j, energy):
        energy = [energy[i] for i in range(planes)]
        for g in range(TILE // (2 * lags)):
            at = pl.multiple_of(j * TILE + g * 2 * lags, 2 * lags)
            pair = [raw[pl.ds(at + h * lags, lags)].reshape(TILE, LANES) for h in (0, 1)]
            out = jnp.dot(sorter[...], jnp.concatenate(pair, axis=1), preferred_element_type=f32)
            for t in range(tiles):
                for d in range(days):
                    i = t * days + d
                    lane = (d % 2) * LANES
                    for h in (0, 1):
                        value = out[i * lags : (i + 1) * lags, h * LANES : (h + 1) * LANES]
                        energy[i] = energy[i] + jnp.sum((value * value).reshape(-1, 8, LANES), axis=0)
                        own[chip ^ t, d // 2, pl.ds(at + h * lags, lags), lane : lane + LANES] = value.astype(own.dtype)
        return jnp.stack(energy)

    def sort_load(j, energy):
        loaded(j).wait()
        energy = sort(j, energy)
        swapped(j).start()
        return energy

    energy = lax.fori_loop(0, last, sort_load, jnp.zeros((planes, 8, LANES), f32))
    loaded(last, lag_count - last * TILE).wait()
    energy = sort(last, energy)
    swapped(last).start()
    swapped_late().start()

    found, used = [], []
    for d in range(days):
        rows = [mask_ref[d : d + 1, t * LANES : (t + 1) * LANES].astype(f32) for t in range(tiles)]
        one = sum(jnp.sum(energy[t * days + d], axis=0, keepdims=True) * rows[t] for t in range(tiles))
        found.append(one)
        used.append(sum(rows))
    stat_out[...] = jnp.concatenate(found + used, axis=0)
    for o in range(1, peers + 1):
        told(o).start()

    def operand(slot, dp):
        return own[mine(slot), dp] if dp < days // 2 else theirs[slot, dp - days // 2]

    def transform(slot, k, dps, target):
        for dp in dps:
            rhs = operand(slot, dp)
            for part in range(CHUNK // TILE):
                start = pl.multiple_of(width - TILE - (k * (CHUNK // TILE) + part) * TILE, TILE)
                target[part * TILE : (part + 1) * TILE, dp * TILE : (dp + 1) * TILE] = jnp.dot(
                    strip[:, pl.ds(start, width)], rhs, preferred_element_type=f32
                )

    def add_days(slot, k, source):
        size = 32
        for row in range(0, CHUNK, size):
            at = pl.multiple_of(k * CHUNK + row, size)
            lin = one = two = jnp.zeros((size // 8, 8, LANES), f32)
            for e in range(2 * days):
                dp, lane = e // 2, (e % 2) * LANES
                if e < days:
                    x = own[mine(slot), dp, pl.ds(at, size), lane : lane + LANES]
                else:
                    x = theirs[slot, dp - days // 2, pl.ds(at, size), lane : lane + LANES]
                x = x.astype(f32).reshape(size // 8, 8, LANES)
                h = source[row : row + size, e * LANES : (e + 1) * LANES].reshape(size // 8, 8, LANES)
                r = lax.rsqrt(x * x + h * h + bias[slot, e][None])
                lin = lin + x * scale[slot, e][None]
                one = one + x * r
                two = two + h * r
            for v, value in enumerate((lin, one, two)):
                sums[v, row : row + size] = value.reshape(size, LANES)

    low_lane = lax.broadcasted_iota(jnp.int32, (ROWS, LANES), 1) < LANES // 2

    def split(half, v, c):
        a = sums[v, half * HALF : half * HALF + ROWS]
        b = sums[v, half * HALF + ROWS : (half + 1) * HALF]
        if c == 0:
            return jnp.where(low_lane, a, pltpu.roll(b, LANES // 2, 1))
        return jnp.where(low_lane, pltpu.roll(a, LANES // 2, 1), b)

    def encode(target, values):
        codes_of, units = [], []
        for value in values:
            top = jnp.max(jnp.abs(value), axis=0, keepdims=True)
            unit = (top * UNIT).astype(jnp.int32) + 1
            step = FULL * UNIT / unit.astype(f32)
            codes_of.append((value * step + 32768.5).astype(jnp.int32))
            units.append(unit)
        lin, one, two = codes_of
        target[:ROWS] = one * 65536 + two
        target[ROWS:WORDS] = lin[: ROWS // 2] * 65536 + lin[ROWS // 2 :]
        pick = lax.broadcasted_iota(jnp.int32, (8, LANES), 0)
        target[WORDS:] = jnp.where(pick == 0, units[0], jnp.where(pick == 1, units[1], units[2]))

    def decode(source):
        units = source[WORDS:].astype(f32) * (1.0 / (FULL * UNIT))

        def value(code, v):
            return (code.astype(f32) - 32768.0) * units[v : v + 1]

        def pieces(word):
            return lax.shift_right_logical(word, jnp.full_like(word, 16)), word & 65535

        one, two = pieces(source[:ROWS])
        top, bottom = pieces(source[ROWS:WORDS])
        return (jnp.concatenate([value(top, 0), value(bottom, 0)], axis=0), value(one, 1), value(two, 2))

    def reduce_days(s, source):
        slot, k = order(s)
        add_days(slot, k, source)
        for half in (0, 1):
            for c in (0, 1):
                values = [split(half, v, c) for v in range(3)]
                for v in range(3):
                    parts[s, half, c, v] = values[v]
                encode(coded.at[s, half, c], values)

    def send(s):
        slot, k = order(s)

        @pl.when(slot + core == 1)
        def _():
            for c in (0, 1):
                finished(coded.at[s, 1 - core, c], k, 1 - core, c).start()

        @pl.when(slot + core == 0)
        def _():
            for half in (0, 1):
                relayed(s, k, half).start()

        @pl.when(slot + core == 2)
        def _():
            for half in (0, 1):
                handed(s, k, half).start()

    def relay(k):
        relayed(0, k, 0).wait_recv()
        for c in (0, 1):
            far = decode(partial_in.at[k, c])
            encode(relay_out.at[k, c], [parts[near_step(k), core, c, v] + far[v] for v in range(3)])
            finished(relay_out.at[k, c], k, core, c).start()

    for j in range(loads):
        swapped(j).wait_recv()
    dps = range(days)
    strip_copy.wait()
    transform(*order(0), dps, even_h)

    mask_copy.wait_recv()
    for o in range(1, peers + 1):
        told(o).wait_recv()
    ours, other = stat_out[...], jnp.zeros_like(stat_out)
    for o in range(1, peers + 1):
        if o % 2:
            other = other + stat_in[o - 1]
        else:
            ours = ours + stat_in[o - 1]
    for which, stats in enumerate((ours, other)):
        row = jnp.sum(stats, axis=1, keepdims=True)
        power = row[:days] / (lag_count * jnp.maximum(row[days:], 1.0)) + 0.1
        weight = lax.rsqrt(power)
        for slot in (0, 1):
            at = pl.multiple_of((chip ^ mine(slot)) * LANES, LANES)
            usable = (mask_in if which else mask_ref)[:, pl.ds(at, LANES)].astype(f32)
            by_day = weight * usable
            offset = jnp.where(usable > 0.0, 0.25 * power, jnp.inf)
            for d in range(days):
                scale[slot, which * days + d] = jnp.broadcast_to(by_day[d : d + 1], (8, LANES))
                bias[slot, which * days + d] = jnp.broadcast_to(offset[d : d + 1], (8, LANES))
    transform(*order(1), dps[:2], odd_h)
    reduce_days(0, even_h)
    send(0)
    transform(*order(1), dps[2:], odd_h)
    swapped_late().wait_recv()

    def step(i, carry):
        for s, target, source in ((2 * i + 1, even_h, odd_h), (2 * i + 2, odd_h, even_h)):
            transform(*order(s + 1), dps, target)
            reduce_days(s, source)
            send(s)
            if source is odd_h:
                @pl.when(i >= 1)
                def _():
                    relay(i - 1)
        return carry

    lax.fori_loop(0, chunks - 1, step, 0)
    reduce_days(steps - 1, odd_h)
    send(steps - 1)
    lax.fori_loop(chunks - 2, chunks, lambda k, carry: (relay(k), carry)[1], 0)
    one_over = 1.0 / jnp.maximum(counts_ref[...].astype(f32), 1.0)
    inverse[:, : LANES // 2] = one_over
    inverse[:, LANES // 2 :] = one_over

    def gather(k, carry):
        for half in (0, 1):
            @pl.when(core == 0)
            def _():
                handed(0, k, half).wait_recv()

            @pl.when(core == 1)
            def _():
                for v in range(3):
                    total[k, half, v] = parts[chunks + k, half, 1, v]

            for s in (0, 1):
                remote(
                    relay_out.at[k, 0, sent], final_in.at[s, k, half, sent], final_send.at[k, half, 0],
                    final_recv.at[s, k, half], partner,
                ).wait_recv()
                far = decode(final_in.at[s, k, half])
                for v in range(3):
                    total[k, half, v] += far[v]
        return carry

    lax.fori_loop(0, chunks, gather, 0)
    over = inverse[...]
    for k in range(chunks):
        for half in (0, 1):
            lin, one, two = (total[k, half, v] for v in range(3))
            lin = lin * over
            power = lin * ((one * one + two * two) * (over * over))
            for ref, value in ((linear_ref, lin), (weighted_ref, power)):
                turned = value.T
                for part in (0, 1):
                    start = k * CHUNK + half * HALF + part * ROWS
                    stop = min(start + ROWS, lag_count)
                    if stop > start:
                        rows = turned[part * LANES // 2 : (part + 1) * LANES // 2]
                        ref[:, start:stop] = rows[:, : stop - start]

    mask_copy.wait_send()
    swapped_late().wait_send()
    for j in range(loads):
        swapped(j).wait_send()
    for o in range(1, peers + 1):
        told(o).wait_send()
    for k in range(chunks):
        for half in (0, 1):
            for c in (0, 1):
                finished(relay_out.at[k, c], k, half, c).wait_send()

            @pl.when(core == 0)
            def _():
                relayed(0, k, half).wait_send()

            @pl.when(core == 1)
            def _():
                handed(0, k, half).wait_send()


def fast_stack(correlations, mask, counts):
    days, pairs, lag_count = correlations.shape
    owned = pairs // lax.axis_size("day")
    peers = 2 * lax.axis_size("pair") - 1
    tiles = pairs // LANES
    planes = tiles * days
    width = chunked(lag_count)
    chunks, loads = width // CHUNK, width // TILE
    by_lag = correlations.transpose(2, 0, 1).reshape(lag_count, days, tiles, LANES)
    by_lag = by_lag.transpose(0, 2, 1, 3).reshape(lag_count, planes, LANES)
    strip = jnp.asarray(block_strip(lag_count))
    out = jax.ShapeDtypeStruct((owned, lag_count), jnp.float32)
    vmem = pl.BlockSpec(memory_space=pltpu.VMEM)
    hbm = pl.BlockSpec(memory_space=pl.ANY)
    dma = pltpu.SemaphoreType.DMA
    bf16, f32, i32 = jnp.bfloat16, jnp.float32, jnp.int32
    return pl.pallas_call(
        functools.partial(fast_kernel, lag_count),
        in_specs=[hbm, vmem, vmem, hbm, vmem],
        out_specs=(vmem, vmem),
        out_shape=(out, out),
        scratch_shapes=[
            pltpu.VMEM((width, planes, LANES), bf16),
            pltpu.VMEM((tiles, days // 2, width, TILE), bf16),
            pltpu.VMEM((2, days // 2, width, TILE), bf16),
            pltpu.VMEM(strip.shape, bf16),
            pltpu.VMEM((CHUNK, 2 * days * LANES), f32),
            pltpu.VMEM((CHUNK, 2 * days * LANES), f32),
            pltpu.VMEM((3, CHUNK, LANES), f32),
            pltpu.VMEM((2, 2 * days, 8, LANES), f32),
            pltpu.VMEM((2, 2 * days, 8, LANES), f32),
            pltpu.VMEM(mask.shape, i32),
            pltpu.VMEM((2 * days, LANES), f32),
            pltpu.VMEM((peers, 2 * days, LANES), f32),
            pltpu.VMEM((2 * chunks, 2, 2, PACK, LANES), i32),
            pltpu.VMEM((2 * chunks, 2, 2, 3, ROWS, LANES), f32),
            pltpu.VMEM((chunks, 2, PACK, LANES), i32),
            pltpu.VMEM((chunks, 2, PACK, LANES), i32),
            pltpu.VMEM((2, chunks, 2, PACK, LANES), i32),
            pltpu.VMEM((chunks, 2, 3, ROWS, LANES), f32),
            pltpu.VMEM((1, LANES), f32),
            dma((loads,)), dma, dma((loads,)), dma((loads,)), dma, dma, dma, dma, dma((peers,)), dma((peers,)),
            dma((chunks, 2)), dma((chunks,)), dma((chunks, 2, 2)), dma((2, chunks, 2)),
            dma((chunks, 2)), dma((chunks, 2)),
        ],
        compiler_params=pltpu.CompilerParams(
            vmem_limit_bytes=125 * 2**19, collective_id=0, has_side_effects=True
        ),
        name="stack",
    )(by_lag, mask, counts.reshape(1, owned), strip, jnp.asarray(sorting_matrix(planes)))


def shards(correlations, mask, counts):
    days, pairs, lag_count = correlations.shape
    groups = lax.axis_size("day")
    if groups == 8 and days == 4 and pairs == groups // 2 * LANES:
        return fast_stack(correlations, mask, counts)
    linear_sum, power = general_sums(correlations, mask)
    inverse = (1.0 / jnp.maximum(counts.astype(jnp.float32), 1.0))[:, None]
    linear = linear_sum * inverse
    return (linear * (power * (inverse * inverse)), linear)


def solution(mesh):
    placed = (P("day", "pair", None), P("day", "pair"), P(("pair", "day")))
    return jax.shard_map(
        shards,
        mesh=mesh,
        in_specs=placed,
        out_specs=(P(("pair", "day"), None), P(("pair", "day"), None)),
        check_vma=False,
    )
```

```python
import functools

import jax
import jax.numpy as jnp
import numpy as np
from jax import lax
from jax.experimental import pallas as pl
from jax.experimental.pallas import tpu as pltpu
from jax.sharding import PartitionSpec as P

TILE = 256
MESH = pl.DeviceIdType.MESH
FULL = 32767.0
UNIT = 2.0**20


def padded(lag_count):
    return -(-lag_count // TILE) * TILE


def kernel_strip(lag_count):
    f32 = np.float32
    offset = np.arange(lag_count, dtype=np.int32)
    offset = np.where(offset > lag_count // 2, offset - lag_count, offset)
    angle = f32(np.pi) * offset.astype(f32) / f32(lag_count)
    parity = f32(1) - f32(2) * (offset % 2).astype(f32)
    sine = np.where(offset == 0, f32(1), np.sin(angle)).astype(f32)
    kernel = np.where(offset == 0, f32(0), (np.cos(angle) - parity) / (f32(lag_count) * sine))
    width = padded(lag_count)
    index = np.arange(2 * width - TILE)[None, :] - np.arange(TILE)[:, None] - (width - TILE)
    return kernel.astype(f32)[index % lag_count].astype(jnp.bfloat16)


def codes(values):
    top = jnp.max(jnp.abs(values), axis=1, keepdims=True)
    units = (top * UNIT).astype(jnp.int32) + 1
    step = FULL * UNIT / units.astype(jnp.float32)
    return jnp.round(values * step).astype(jnp.int32), units


def join(high, low):
    return high * 65536 + (low & 65535)


def split(word):
    low = ((word & 65535) ^ 32768) - 32768
    return word >> 16, low


def stack_kernel(
    lag_count, x_hbm, mask_ref, strip_hbm, linear_ref, power_ref,
    rows_ref, stage, strip, table, sums, first_hilbert, mask_in, mask_turned, row_mask, day_weight,
    stat_out, stat_in, words_out, words_in,
    load_sem, stage_sem, strip_sem, swap_send, swap_recv, mask_send, mask_recv,
    stat_send, stat_recv, word_send, word_recv,
):
    width = table.shape[1]
    half = width // 2
    chips, all_days, owned, _ = rows_ref.shape
    days = all_days // 2
    total = all_days * owned
    part = owned // 2
    pieces = words_out.shape[0]
    peers = stat_in.shape[0]
    me, plane = lax.axis_index("day"), lax.axis_index("pair")
    chip, core = me // 2, me % 2
    partner = {"day": me ^ 1, "pair": plane}
    last = width - TILE
    tiles = [slice(j * TILE, min((j + 1) * TILE, lag_count)) for j in range(width // TILE)]

    def mine(g):
        return pltpu.make_async_copy(x_hbm.at[:, 2 * g + core], rows_ref.at[g, pl.ds(0, days)], load_sem.at[g])

    def staged(g):
        return pltpu.make_async_copy(x_hbm.at[:, 2 * g + 1 - core], stage.at[g], stage_sem.at[g])

    def swapped(g):
        return pltpu.make_async_remote_copy(
            stage.at[g], rows_ref.at[g, pl.ds(days, days)], swap_send.at[g], swap_recv.at[g],
            device_id=partner, device_id_type=MESH,
        )

    def peer(o):
        rank = (2 * plane + core + o) % (peers + 1)
        return {"day": 2 * chip + rank % 2, "pair": rank // 2}

    def told(o):
        return pltpu.make_async_remote_copy(
            stat_out, stat_in.at[o - 1], stat_send.at[o - 1], stat_recv.at[o - 1],
            device_id=peer(o), device_id_type=MESH,
        )

    def owner(o):
        return {"day": 2 * (chip ^ o) + core, "pair": plane}

    def shipped(piece, o):
        return pltpu.make_async_remote_copy(
            words_out.at[piece], words_in.at[piece], word_send.at[piece], word_recv.at[piece],
            device_id=owner(o), device_id_type=MESH,
        )

    far = range(chips - 1, 3, -1)
    order = [chip ^ o for o in (3, *far, 1, 2, 0)]
    strip_copy = pltpu.make_async_copy(strip_hbm, strip, strip_sem)
    strip_copy.start()
    for g in order:
        staged(g).start()
        mine(g).start()

    barrier = pltpu.get_barrier_semaphore()
    for o in range(1, peers + 1):
        pl.semaphore_signal(barrier, inc=1, device_id=peer(o), device_id_type=MESH)
    for o in range(1, chips):
        pl.semaphore_signal(barrier, inc=1, device_id=owner(o), device_id_type=MESH)
    strip_copy.wait()
    for i in range(width // TILE):
        start = width - TILE - i * TILE
        table[pl.ds(i * TILE, TILE), :] = strip[:, start : start + width]
    sums[:, :, last:] = jnp.zeros((3, owned, TILE), jnp.float32)
    pl.semaphore_wait(barrier, peers + chips - 1)

    mask_copy = pltpu.make_async_remote_copy(
        mask_ref, mask_in, mask_send, mask_recv, device_id=partner, device_id_type=MESH
    )
    mask_copy.start()
    for g in order:
        staged(g).wait()
        swapped(g).start()
    mask_copy.wait_recv()
    both_masks = jnp.concatenate([mask_ref[...], mask_in[...]], axis=0).astype(jnp.float32)
    mask_turned[...] = both_masks.T

    def mask_rows(block, count):
        rows = mask_turned[pl.ds(pl.multiple_of(block * owned, owned), owned), :]
        return jnp.concatenate([rows[:, d : d + 1] for d in range(count)], axis=0)

    def statistics(step, carry):
        g = chip ^ (chips - 1 - step)
        mine(g).wait()
        of_pairs = mask_rows(2 * g + core, all_days)
        row_mask[g] = of_pairs.reshape(all_days, owned, 1)
        for x_ref, rows in ((rows_ref.at[g, pl.ds(0, days)], of_pairs[: days * owned]),
                            (stage.at[g], mask_rows(2 * g + 1 - core, days))):
            x = x_ref[...].reshape(days * owned, lag_count).astype(jnp.float32)
            energy = jnp.sum(x * x, axis=1, keepdims=True) * rows
            both = jnp.concatenate(
                [jnp.broadcast_to(energy, (days * owned, 128)), jnp.broadcast_to(rows, (days * owned, 128))], axis=1
            )
            carry = carry + jnp.sum(both.reshape(days, owned, 256), axis=1)
        return carry

    found = lax.fori_loop(0, chips, statistics, jnp.zeros((days, 256), jnp.float32))
    none = jnp.zeros_like(found)
    stat_out[...] = jnp.where(
        core == 0, jnp.concatenate([found, none], axis=0), jnp.concatenate([none, found], axis=0)
    )
    for o in range(1, peers + 1):
        told(o).start()

    def transform(g, here, cols):
        lhs = rows_ref[g, :, here, :].reshape(-1, lag_count)
        return jnp.dot(lhs, table[:lag_count, cols], preferred_element_type=jnp.float32)

    def add_days(g, here, cols, hilbert):
        size = cols.stop - cols.start
        count = hilbert.shape[0] // all_days
        scale = (day_weight[:, :count] * row_mask[g, :, here, :]).reshape(-1, 1)
        real = scale * rows_ref[g, :, here, cols].reshape(-1, size).astype(jnp.float32)
        imag = scale * hilbert
        inverse = lax.rsqrt(real * real + imag * imag + 0.25)
        for k, term in enumerate((real, real * inverse, imag * inverse)):
            sums[k, :count, cols] = jnp.sum(term.reshape(all_days, count, size), axis=0)

    def encode(piece, rows, o):
        linear, linear_units = codes(sums[0, rows])
        first, first_units = codes(sums[1, rows])
        second, second_units = codes(sums[2, rows])
        words_out[piece, :, :width] = join(first, second)
        words_out[piece, :, width : width + half] = join(linear[:, :half], linear[:, half:])
        pick = lax.broadcasted_iota(jnp.int32, (part, 128), 1)
        words_out[piece, :, width + half :] = jnp.where(
            pick == 0, linear_units, jnp.where(pick == 1, first_units, second_units)
        )
        shipped(piece, o).start()

    def decode(piece, rows):
        units = words_in[piece, :, width + half :].astype(jnp.float32) * (1.0 / (FULL * UNIT))
        left, right = split(words_in[piece, :, width : width + half])
        sums[0, rows, :half] += left.astype(jnp.float32) * units[:, 0:1]
        sums[0, rows, half:] += right.astype(jnp.float32) * units[:, 0:1]
        first, second = split(words_in[piece, :, :width])
        sums[1, rows] += first.astype(jnp.float32) * units[:, 1:2]
        sums[2, rows] += second.astype(jnp.float32) * units[:, 2:3]

    whole, low, high = pl.ds(0, owned), pl.ds(0, part), pl.ds(part, part)

    swapped(order[0]).wait_recv()
    for cols in tiles:
        first_hilbert[:, cols] = transform(order[0], whole, cols)

    for o in range(1, peers + 1):
        told(o).wait_recv()
    stats = stat_out[...]
    for o in range(peers):
        stats = stats + stat_in[o]
    weight = lax.rsqrt(stats[:, :128] / (lag_count * jnp.maximum(stats[:, 128:], 1.0)) + 0.1)
    weight = jnp.where(core == 0, weight, jnp.concatenate([weight[days:], weight[:days]], axis=0))
    for d in range(all_days):
        day_weight[d] = jnp.broadcast_to(weight[d : d + 1, :1], (owned, 1))

    for cols in tiles:
        add_days(order[0], whole, cols, first_hilbert[:, cols])
    encode(0, low, 1)
    encode(1, high, 2)

    def far_block(step, carry):
        o = chips - 1 - step
        swapped(chip ^ o).wait_recv()
        for cols in tiles:
            add_days(chip ^ o, whole, cols, transform(chip ^ o, whole, cols))
        encode(2 * o - 2, low, o)
        encode(2 * o - 1, high, o)
        return carry

    if chips > 4:
        lax.fori_loop(0, chips - 4, far_block, 0)

    def near_half(q, carry):
        o = 1 + q % 2
        g = chip ^ o
        here = pl.ds(pl.multiple_of(((q + q // 2) % 2) * part, part), part)

        @pl.when(q < 2)
        def _():
            swapped(g).wait_recv()

        for cols in tiles:
            add_days(g, here, cols, transform(g, here, cols))

        @pl.when(q >= 2)
        def _():
            shipped(3 - q, o).wait_recv()
            decode(3 - q, low)

        encode(2 + q, low, o)
        return carry

    lax.fori_loop(0, 4, near_half, 0)
    swapped(chip).wait_recv()
    for cols in tiles:
        add_days(chip, whole, cols, transform(chip, whole, cols))

    def arrive(piece, carry):
        turn = piece + jnp.where(piece // 2 == 2, 1, 0)
        shipped(piece, 1).wait_recv()
        decode(piece, pl.ds(pl.multiple_of((turn % 2) * part, part), part))
        return carry

    lax.fori_loop(2, pieces, arrive, 0)
    real, imag = sums[1, :, :lag_count], sums[2, :, :lag_count]
    linear_ref[...] = sums[0, :, :lag_count]
    power_ref[...] = real * real + imag * imag

    mask_copy.wait_send()
    for g in range(chips):
        swapped(g).wait_send()
    for o in range(1, peers + 1):
        told(o).wait_send()
    for piece in range(pieces):
        shipped(piece, 1).wait_send()


def general_sums(correlations, mask):
    days, pairs, lag_count = correlations.shape
    groups = lax.axis_size("day")
    chips = groups // 2
    owned = pairs // groups
    width = padded(lag_count)
    peers = 2 * lax.axis_size("pair") - 1

    strip = jnp.asarray(kernel_strip(lag_count))
    size = width + width // 2 + 128
    pieces = 2 * chips - 2
    out = jax.ShapeDtypeStruct((owned, lag_count), jnp.float32)
    vmem = pl.BlockSpec(memory_space=pltpu.VMEM)
    hbm = pl.BlockSpec(memory_space=pl.ANY)
    dma = pltpu.SemaphoreType.DMA
    return pl.pallas_call(
        functools.partial(stack_kernel, lag_count),
        in_specs=[hbm, vmem, hbm],
        out_specs=(vmem, vmem),
        out_shape=(out, out),
        scratch_shapes=[
            pltpu.VMEM((chips, 2 * days, owned, lag_count), jnp.bfloat16),
            pltpu.VMEM((chips, days, owned, lag_count), jnp.bfloat16),
            pltpu.VMEM(strip.shape, jnp.bfloat16),
            pltpu.VMEM((width, width), jnp.bfloat16),
            pltpu.VMEM((3, owned, width), jnp.float32),
            pltpu.VMEM((2 * days * owned, width), jnp.float32),
            pltpu.VMEM((days, pairs), jnp.int32),
            pltpu.VMEM((pairs, 2 * days), jnp.float32),
            pltpu.VMEM((chips, 2 * days, owned, 1), jnp.float32),
            pltpu.VMEM((2 * days, owned, 1), jnp.float32),
            pltpu.VMEM((2 * days, 256), jnp.float32),
            pltpu.VMEM((peers, 2 * days, 256), jnp.float32),
            pltpu.VMEM((pieces, owned // 2, size), jnp.int32),
            pltpu.VMEM((pieces, owned // 2, size), jnp.int32),
            dma((chips,)), dma((chips,)), dma, dma((chips,)), dma((chips,)), dma, dma,
            dma((peers,)), dma((peers,)), dma((pieces,)), dma((pieces,)),
        ],
        compiler_params=pltpu.CompilerParams(
            vmem_limit_bytes=46 * 2**20, collective_id=0, has_side_effects=True
        ),
        name="stack",
    )(correlations.reshape(days, groups, owned, lag_count), mask, strip)


LANES = 128
CHUNK = 512
HALF = CHUNK // 2
ROWS = HALF // 2
WORDS = ROWS + ROWS // 2
PACK = WORDS + 8
SENT = WORDS + 3


def block_strip(lag_count):
    f32 = np.float32
    offset = np.arange(lag_count, dtype=np.int32)
    offset = np.where(offset > lag_count // 2, offset - lag_count, offset)
    angle = f32(np.pi) * offset.astype(f32) / f32(lag_count)
    parity = f32(1) - f32(2) * (offset % 2).astype(f32)
    sine = np.where(offset == 0, f32(1), np.sin(angle)).astype(f32)
    kernel = np.where(offset == 0, f32(0), (np.cos(angle) - parity) / (f32(lag_count) * sine))
    width = chunked(lag_count)
    index = np.arange(TILE)[:, None] - np.arange(2 * width - TILE)[None, :] + (width - TILE)
    return kernel.astype(f32)[index % lag_count].astype(jnp.bfloat16)


def chunked(lag_count):
    return -(-lag_count // CHUNK) * CHUNK


def sorting_matrix(rows):
    lags = TILE // rows
    out = np.arange(TILE)
    source = (out % lags) * rows + out // lags
    return (source[:, None] == np.arange(TILE)[None, :]).astype(jnp.bfloat16)


def fast_kernel(
    lag_count, x_hbm, mask_hbm, counts_hbm, strip_hbm, sorter_hbm, power_ref, linear_ref, inverse_ref,
    mask_ref, counts_ref, sorter, raw, own, theirs, strip, even_h, odd_h, sums, scale, bias, mask_in, stat_out, stat_in,
    coded, parts, partial_in, relay_out, final_in, total,
    load_sem, small_sem, swap_send, swap_recv, late_send, late_recv, mask_send, mask_recv, stat_send, stat_recv,
    partial_send, partial_recv, final_send, final_recv, own_send, own_recv,
):
    f32 = jnp.float32
    width = raw.shape[0]
    planes = raw.shape[1]
    loads = width // TILE
    chunks = width // CHUNK
    steps = 2 * chunks
    peers = stat_in.shape[0]
    days = mask_ref.shape[0]
    tiles = mask_ref.shape[1] // LANES
    lags = TILE // planes
    me, plane = lax.axis_index("day"), lax.axis_index("pair")
    chip, core = me // 2, me % 2
    partner = {"day": me ^ 1, "pair": plane}

    def pick(s, table):
        return sum(jnp.where(s == i, value, 0) for i, value in enumerate(table))

    def order(s):
        return (
            jnp.where(core == 0, pick(s, (0, 0, 0, 1, 0, 1, 1, 1)), s // chunks),
            jnp.where(core == 0, pick(s, (0, 2, 1, 0, 3, 1, 2, 3)), pick(s, (2, 3, 0, 1, 0, 1, 2, 3))),
        )

    def near(o, c):
        return {"day": 2 * (chip ^ o) + c, "pair": plane}

    def peer(o):
        rank = (2 * plane + core + o) % (peers + 1)
        return {"day": 2 * chip + rank % 2, "pair": rank // 2}

    def loaded(j, count=TILE):
        rows = pl.ds(j * TILE, count)
        return pltpu.make_async_copy(x_hbm.at[rows], raw.at[rows], load_sem.at[j])

    def remote(source, target, send, recv, device):
        return pltpu.make_async_remote_copy(
            source, target, send, recv, device_id=device, device_id_type=MESH
        )

    def mine(slot):
        return 2 * (1 - core) + 1 - slot

    def swapped(j):
        rows = pl.ds(pl.multiple_of(j * TILE, TILE), TILE)
        return remote(
            own.at[2 * core + 1, :, rows], theirs.at[0, :, rows], swap_send.at[j], swap_recv.at[j], partner
        )

    def swapped_late():
        return remote(own.at[2 * core], theirs.at[1], late_send, late_recv, partner)

    def told(o):
        return remote(stat_out, stat_in.at[o - 1], stat_send.at[o - 1], stat_recv.at[o - 1], peer(o))

    sent = pl.ds(0, SENT)

    def relayed(s, k, half):
        far = k // 2
        return remote(
            coded.at[s, half, :, sent], partial_in.at[k % 2, half, :, sent], partial_send.at[k, half],
            partial_recv.at[k % 2, half], near(2 - far, 1 - far),
        )

    def finished(source, k, half, c):
        return remote(
            source.at[sent], final_in.at[1 - core, k, half, sent], final_send.at[k, half, c],
            final_recv.at[1 - core, k, half], near(2 - core, c),
        )

    def handed(s, k, half):
        return remote(
            parts.at[s, half, 0], total.at[k, half], own_send.at[k, half], own_recv.at[k, half], partner
        )

    last = loads - 1
    small = [
        pltpu.make_async_copy(source, target, small_sem.at[i])
        for i, (source, target) in enumerate(
            ((sorter_hbm, sorter), (mask_hbm, mask_ref), (counts_hbm, counts_ref), (strip_hbm, strip))
        )
    ]
    for copy in small[:3]:
        copy.start()
    for j in range(last):
        loaded(j).start()
    loaded(last, lag_count - last * TILE).start()
    small[3].start()
    barrier = pltpu.get_barrier_semaphore()
    for o in range(1, peers + 1):
        pl.semaphore_signal(barrier, inc=1, device_id=peer(o), device_id_type=MESH)
    for o in (1, 2):
        for c in (0, 1):
            pl.semaphore_signal(barrier, inc=1, device_id=near(o, c), device_id_type=MESH)
    raw[lag_count:] = jnp.zeros((width - lag_count, planes, LANES), raw.dtype)
    pl.semaphore_wait(barrier, peers + 4)
    small[0].wait()
    small[1].wait()
    mask_copy = remote(mask_ref, mask_in, mask_send, mask_recv, partner)
    mask_copy.start()

    def sort(j, energy):
        energy = [energy[i] for i in range(planes)]
        for g in range(TILE // (2 * lags)):
            at = pl.multiple_of(j * TILE + g * 2 * lags, 2 * lags)
            pair = [raw[pl.ds(at + h * lags, lags)].reshape(TILE, LANES) for h in (0, 1)]
            out = jnp.dot(sorter[...], jnp.concatenate(pair, axis=1), preferred_element_type=f32)
            for t in range(tiles):
                for d in range(days):
                    i = t * days + d
                    lane = (d % 2) * LANES
                    for h in (0, 1):
                        value = out[i * lags : (i + 1) * lags, h * LANES : (h + 1) * LANES]
                        energy[i] = energy[i] + jnp.sum((value * value).reshape(-1, 8, LANES), axis=0)
                        own[chip ^ t, d // 2, pl.ds(at + h * lags, lags), lane : lane + LANES] = value.astype(own.dtype)
        return jnp.stack(energy)

    def sort_load(j, energy):
        loaded(j).wait()
        energy = sort(j, energy)
        swapped(j).start()
        return energy

    energy = lax.fori_loop(0, last, sort_load, jnp.zeros((planes, 8, LANES), f32))
    loaded(last, lag_count - last * TILE).wait()
    energy = sort(last, energy)
    swapped(last).start()
    swapped_late().start()

    found, used = [], []
    for d in range(days):
        rows = [mask_ref[d : d + 1, t * LANES : (t + 1) * LANES].astype(f32) for t in range(tiles)]
        one = sum(jnp.sum(energy[t * days + d], axis=0, keepdims=True) * rows[t] for t in range(tiles))
        found.append(one)
        used.append(sum(rows))
    stat_out[...] = jnp.concatenate(found + used, axis=0)
    for o in range(1, peers + 1):
        told(o).start()

    def operand(slot, dp):
        return own[mine(slot), dp] if dp < days // 2 else theirs[slot, dp - days // 2]

    parts_of = CHUNK // TILE

    def transform_piece(slot, k, piece, target):
        dp, part = piece // parts_of, piece % parts_of
        start = pl.multiple_of(width - TILE - (k * parts_of + part) * TILE, TILE)
        target[part * TILE : (part + 1) * TILE, dp * TILE : (dp + 1) * TILE] = jnp.dot(
            strip[:, pl.ds(start, width)], operand(slot, dp), preferred_element_type=f32
        )

    def transform(slot, k, pieces, target):
        for piece in pieces:
            transform_piece(slot, k, piece, target)

    def add_days(slot, k, first, stop, source):
        size = 32
        for row in range(first, stop, size):
            at = pl.multiple_of(k * CHUNK + row, size)
            lin = one = two = jnp.zeros((size // 8, 8, LANES), f32)
            for e in range(2 * days):
                dp, lane = e // 2, (e % 2) * LANES
                if e < days:
                    x = own[mine(slot), dp, pl.ds(at, size), lane : lane + LANES]
                else:
                    x = theirs[slot, dp - days // 2, pl.ds(at, size), lane : lane + LANES]
                x = x.astype(f32).reshape(size // 8, 8, LANES)
                h = source[row : row + size, e * LANES : (e + 1) * LANES].reshape(size // 8, 8, LANES)
                r = lax.rsqrt(x * x + h * h + bias[slot, e][None])
                lin = lin + x * scale[slot, e][None]
                one = one + x * r
                two = two + h * r
            for v, value in enumerate((lin, one, two)):
                sums[v, row : row + size] = value.reshape(size, LANES)

    low_lane = lax.broadcasted_iota(jnp.int32, (ROWS, LANES), 1) < LANES // 2

    def split(half, v, c):
        a = sums[v, half * HALF : half * HALF + ROWS]
        b = sums[v, half * HALF + ROWS : (half + 1) * HALF]
        if c == 0:
            return jnp.where(low_lane, a, pltpu.roll(b, LANES // 2, 1))
        return jnp.where(low_lane, pltpu.roll(a, LANES // 2, 1), b)

    def encode(target, values):
        codes_of, units = [], []
        for value in values:
            top = jnp.max(jnp.abs(value), axis=0, keepdims=True)
            unit = (top * UNIT).astype(jnp.int32) + 1
            step = FULL * UNIT / unit.astype(f32)
            codes_of.append((value * step + 32768.5).astype(jnp.int32))
            units.append(unit)
        lin, one, two = codes_of
        target[:ROWS] = one * 65536 + two
        target[ROWS:WORDS] = lin[: ROWS // 2] * 65536 + lin[ROWS // 2 :]
        pick = lax.broadcasted_iota(jnp.int32, (8, LANES), 0)
        target[WORDS:] = jnp.where(pick == 0, units[0], jnp.where(pick == 1, units[1], units[2]))

    def decode(source):
        units = source[WORDS:].astype(f32) * (1.0 / (FULL * UNIT))

        def value(code, v):
            return (code.astype(f32) - 32768.0) * units[v : v + 1]

        def pieces(word):
            return lax.shift_right_logical(word, jnp.full_like(word, 16)), word & 65535

        one, two = pieces(source[:ROWS])
        top, bottom = pieces(source[ROWS:WORDS])
        return (jnp.concatenate([value(top, 0), value(bottom, 0)], axis=0), value(one, 1), value(two, 2))

    def code(s, half, c):
        values = [split(half, v, c) for v in range(3)]
        for v in range(3):
            parts[s, half, c, v] = values[v]
        encode(coded.at[s, half, c], values)

    def step_both(s, source, target):
        slot, k = order(s)
        rows = (0, 96, 192, 288, 384, 448, CHUNK)
        for piece in range(2 * days):
            if piece < len(rows) - 1:
                add_days(slot, k, rows[piece], rows[piece + 1], source)
            if piece in (3, 4):
                code(s, 0, piece - 3)
            if piece in (6, 7):
                code(s, 1, piece - 6)
            if target is not None:
                transform_piece(*order(s + 1), piece, target)

    def send(s, halves=(0, 1)):
        slot, k = order(s)

        @pl.when(jnp.logical_and(slot + core == 1, k // 2 == core))
        def _():
            for half in halves:
                for c in (0, 1):
                    finished(coded.at[s, half, c], k, half, c).start()

        @pl.when(slot + core == 0)
        def _():
            for half in halves:
                relayed(s, k, half).start()

        @pl.when(slot + core == 2)
        def _():
            for half in halves:
                handed(s, k, half).start()

    def relay(r):
        k = r + 2 * (1 - core)
        s = r + jnp.where(core == 0, steps - 2, 2)
        def one(half, carry):
            relayed(0, r, half).wait_recv()
            for c in (0, 1):
                far = decode(partial_in.at[r, half, c])
                encode(relay_out.at[r, half, c], [parts[s, half, c, v] + far[v] for v in range(3)])
                finished(relay_out.at[r, half, c], k, half, c).start()
            return carry

        lax.fori_loop(0, 2, one, 0)

    for j in range(loads):
        swapped(j).wait_recv()
    small[3].wait()
    transform(*order(0), range(2 * days), even_h)
    transform(*order(1), range(days), odd_h)

    mask_copy.wait_recv()
    for o in range(1, peers + 1):
        told(o).wait_recv()
    ours, other = stat_out[...], jnp.zeros_like(stat_out)
    for o in range(1, peers + 1):
        if o % 2:
            other = other + stat_in[o - 1]
        else:
            ours = ours + stat_in[o - 1]
    for which, stats in enumerate((ours, other)):
        row = jnp.sum(stats, axis=1, keepdims=True)
        power = row[:days] / (lag_count * jnp.maximum(row[days:], 1.0)) + 0.1
        weight = lax.rsqrt(power)
        for slot in (0, 1):
            at = pl.multiple_of((chip ^ mine(slot)) * LANES, LANES)
            usable = (mask_in if which else mask_ref)[:, pl.ds(at, LANES)].astype(f32)
            by_day = weight * usable
            offset = jnp.where(usable > 0.0, 0.25 * power, jnp.inf)
            for d in range(days):
                scale[slot, which * days + d] = jnp.broadcast_to(by_day[d : d + 1], (8, LANES))
                bias[slot, which * days + d] = jnp.broadcast_to(offset[d : d + 1], (8, LANES))
    for half in (0, 1):
        for i in range(2):
            first = half * HALF + i * ROWS
            add_days(*order(0), first, first + ROWS, even_h)
            if i:
                code(0, half, 0)
                code(0, half, 1)
            transform_piece(*order(1), days + 2 * half + i, odd_h)
        send(0, (half,))
    swapped_late().wait_recv()

    def step(i, carry):
        for s, target, source in ((2 * i + 1, even_h, odd_h), (2 * i + 2, odd_h, even_h)):
            step_both(s, source, target)
            send(s)
            if source is odd_h:
                @pl.when(jnp.logical_and(core == 1, i >= 1))
                def _():
                    relay(i - 1)
            else:
                @pl.when(jnp.logical_and(core == 0, i == chunks - 2))
                def _():
                    relay(0)
        return carry

    lax.fori_loop(0, chunks - 1, step, 0)
    step_both(steps - 1, odd_h, None)
    send(steps - 1)

    @pl.when(core == 0)
    def _():
        relay(1)

    small[2].wait()
    inverse_ref[...] = 1.0 / jnp.maximum(counts_ref[...].astype(f32), 1.0)

    @pl.when(core == 0)
    def _():
        for k in range(chunks):
            for half in (0, 1):
                handed(0, k, half).wait_recv()

    @pl.when(core == 1)
    def _():
        def keep(k, carry):
            for half in (0, 1):
                for v in range(3):
                    total[k, half, v] = parts[chunks + k, half, 1, v]
            return carry

        lax.fori_loop(0, chunks, keep, 0)

    def settle():
        mask_copy.wait_send()
        swapped_late().wait_send()
        for j in range(loads):
            swapped(j).wait_send()
        for o in range(1, peers + 1):
            told(o).wait_send()
        for k in range(chunks):
            for half in (0, 1):
                for c in (0, 1):
                    finished(relay_out.at[0, 0, 0], k, half, c).wait_send()

            @pl.when(core == 0)
            def _():
                for half in (0, 1):
                    relayed(0, k, half).wait_send()

            @pl.when(core == 1)
            def _():
                for half in (0, 1):
                    handed(0, k, half).wait_send()

    seen = set()
    for s, k in ((0, 2), (1, 0), (0, 3), (1, 1), (0, 0), (1, 2), (0, 1), (1, 3)):
        if (s, k) == (1, 3):
            settle()
        for half in (0, 1):
            remote(
                relay_out.at[0, 0, 0, sent], final_in.at[s, k, half, sent], final_send.at[k, half, 0],
                final_recv.at[s, k, half], partner,
            ).wait_recv()
            found = decode(final_in.at[s, k, half])
            if k not in seen:
                for v in range(3):
                    total[k, half, v] += found[v]
                continue
            lin, one, two = (total[k, half, v] + found[v] for v in range(3))
            for ref, value in ((linear_ref, lin), (power_ref, one * one + two * two)):
                turned = value.T
                for part in (0, 1):
                    start = k * CHUNK + half * HALF + part * ROWS
                    stop = min(start + ROWS, lag_count)
                    if stop > start:
                        rows = turned[part * LANES // 2 : (part + 1) * LANES // 2]
                        ref[:, start:stop] = rows[:, : stop - start]
        seen.add(k)


def fast_stack(correlations, mask, counts):
    days, pairs, lag_count = correlations.shape
    owned = pairs // lax.axis_size("day")
    peers = 2 * lax.axis_size("pair") - 1
    tiles = pairs // LANES
    planes = tiles * days
    width = chunked(lag_count)
    chunks, loads = width // CHUNK, width // TILE
    by_lag = correlations.transpose(2, 0, 1).reshape(lag_count, days, tiles, LANES)
    by_lag = by_lag.transpose(0, 2, 1, 3).reshape(lag_count, planes, LANES)
    strip = jnp.asarray(block_strip(lag_count))
    sorter = jnp.asarray(sorting_matrix(planes))
    out = jax.ShapeDtypeStruct((owned, lag_count), jnp.float32)
    vmem = pl.BlockSpec(memory_space=pltpu.VMEM)
    hbm = pl.BlockSpec(memory_space=pltpu.HBM)
    dma = pltpu.SemaphoreType.DMA
    bf16, f32, i32 = jnp.bfloat16, jnp.float32, jnp.int32
    power, linear_sum, inverse = pl.pallas_call(
        functools.partial(fast_kernel, lag_count),
        in_specs=[hbm] * 5,
        out_specs=(vmem, vmem, vmem),
        out_shape=(out, out, jax.ShapeDtypeStruct((1, owned), f32)),
        scratch_shapes=[
            pltpu.VMEM(mask.shape, i32),
            pltpu.VMEM((1, owned), i32),
            pltpu.VMEM(sorter.shape, bf16),
            pltpu.VMEM((width, planes, LANES), bf16),
            pltpu.VMEM((tiles, days // 2, width, TILE), bf16),
            pltpu.VMEM((2, days // 2, width, TILE), bf16),
            pltpu.VMEM(strip.shape, bf16),
            pltpu.VMEM((CHUNK, 2 * days * LANES), f32),
            pltpu.VMEM((CHUNK, 2 * days * LANES), f32),
            pltpu.VMEM((3, CHUNK, LANES), f32),
            pltpu.VMEM((2, 2 * days, 8, LANES), f32),
            pltpu.VMEM((2, 2 * days, 8, LANES), f32),
            pltpu.VMEM(mask.shape, i32),
            pltpu.VMEM((2 * days, LANES), f32),
            pltpu.VMEM((peers, 2 * days, LANES), f32),
            pltpu.VMEM((2 * chunks, 2, 2, PACK, LANES), i32),
            pltpu.VMEM((2 * chunks, 2, 2, 3, ROWS, LANES), f32),
            pltpu.VMEM((2, 2, 2, PACK, LANES), i32),
            pltpu.VMEM((2, 2, 2, PACK, LANES), i32),
            pltpu.VMEM((2, chunks, 2, PACK, LANES), i32),
            pltpu.VMEM((chunks, 2, 3, ROWS, LANES), f32),
            dma((loads,)), dma((4,)), dma((loads,)), dma((loads,)), dma, dma, dma, dma, dma((peers,)), dma((peers,)),
            dma((chunks, 2)), dma((2, 2)), dma((chunks, 2, 2)), dma((2, chunks, 2)),
            dma((chunks, 2)), dma((chunks, 2)),
        ],
        compiler_params=pltpu.CompilerParams(
            vmem_limit_bytes=46 * 2**20, collective_id=0, has_side_effects=True
        ),
        name="stack",
    )(*(pltpu.with_memory_space_constraint(v, pltpu.HBM) for v in (by_lag, mask, counts.reshape(1, owned), strip, sorter)))
    return linear_sum, power, inverse.reshape(owned, 1)


def shards(correlations, mask, counts):
    days, pairs, lag_count = correlations.shape
    groups = lax.axis_size("day")
    four = groups == 8 and days == 4 and chunked(lag_count) == 4 * CHUNK
    if four and pairs == 4 * LANES:
        linear_sum, power, inverse = fast_stack(correlations, mask, counts)
    else:
        linear_sum, power = general_sums(correlations, mask)
        inverse = (1.0 / jnp.maximum(counts.astype(jnp.float32), 1.0))[:, None]
    linear = linear_sum * inverse
    return (linear * (power * (inverse * inverse)), linear)


def solution(mesh):
    placed = (P("day", "pair", None), P("day", "pair"), P(("pair", "day")))
    return jax.shard_map(
        shards,
        mesh=mesh,
        in_specs=placed,
        out_specs=(P(("pair", "day"), None), P(("pair", "day"), None)),
        check_vma=False,
    )
```

```python
import functools

import jax
import jax.numpy as jnp
import numpy as np
from jax import lax
from jax.experimental import pallas as pl
from jax.experimental.pallas import tpu as pltpu
from jax.sharding import PartitionSpec as P

TILE = 256
MESH = pl.DeviceIdType.MESH
FULL = 32767.0
UNIT = 2.0**20


def padded(lag_count):
    return -(-lag_count // TILE) * TILE


def kernel_strip(lag_count):
    f32 = np.float32
    offset = np.arange(lag_count, dtype=np.int32)
    offset = np.where(offset > lag_count // 2, offset - lag_count, offset)
    angle = f32(np.pi) * offset.astype(f32) / f32(lag_count)
    parity = f32(1) - f32(2) * (offset % 2).astype(f32)
    sine = np.where(offset == 0, f32(1), np.sin(angle)).astype(f32)
    kernel = np.where(offset == 0, f32(0), (np.cos(angle) - parity) / (f32(lag_count) * sine))
    width = padded(lag_count)
    index = np.arange(2 * width - TILE)[None, :] - np.arange(TILE)[:, None] - (width - TILE)
    return kernel.astype(f32)[index % lag_count].astype(jnp.bfloat16)


def codes(values):
    top = jnp.max(jnp.abs(values), axis=1, keepdims=True)
    units = (top * UNIT).astype(jnp.int32) + 1
    step = FULL * UNIT / units.astype(jnp.float32)
    return jnp.round(values * step).astype(jnp.int32), units


def join(high, low):
    return high * 65536 + (low & 65535)


def split(word):
    low = ((word & 65535) ^ 32768) - 32768
    return word >> 16, low


def stack_kernel(
    lag_count, x_hbm, mask_ref, strip_hbm, linear_ref, power_ref,
    rows_ref, stage, strip, table, sums, first_hilbert, mask_in, mask_turned, row_mask, day_weight,
    stat_out, stat_in, words_out, words_in,
    load_sem, stage_sem, strip_sem, swap_send, swap_recv, mask_send, mask_recv,
    stat_send, stat_recv, word_send, word_recv,
):
    width = table.shape[1]
    half = width // 2
    chips, all_days, owned, _ = rows_ref.shape
    days = all_days // 2
    total = all_days * owned
    part = owned // 2
    pieces = words_out.shape[0]
    peers = stat_in.shape[0]
    me, plane = lax.axis_index("day"), lax.axis_index("pair")
    chip, core = me // 2, me % 2
    partner = {"day": me ^ 1, "pair": plane}
    last = width - TILE
    tiles = [slice(j * TILE, min((j + 1) * TILE, lag_count)) for j in range(width // TILE)]

    def mine(g):
        return pltpu.make_async_copy(x_hbm.at[:, 2 * g + core], rows_ref.at[g, pl.ds(0, days)], load_sem.at[g])

    def staged(g):
        return pltpu.make_async_copy(x_hbm.at[:, 2 * g + 1 - core], stage.at[g], stage_sem.at[g])

    def swapped(g):
        return pltpu.make_async_remote_copy(
            stage.at[g], rows_ref.at[g, pl.ds(days, days)], swap_send.at[g], swap_recv.at[g],
            device_id=partner, device_id_type=MESH,
        )

    def peer(o):
        rank = (2 * plane + core + o) % (peers + 1)
        return {"day": 2 * chip + rank % 2, "pair": rank // 2}

    def told(o):
        return pltpu.make_async_remote_copy(
            stat_out, stat_in.at[o - 1], stat_send.at[o - 1], stat_recv.at[o - 1],
            device_id=peer(o), device_id_type=MESH,
        )

    def owner(o):
        return {"day": 2 * (chip ^ o) + core, "pair": plane}

    def shipped(piece, o):
        return pltpu.make_async_remote_copy(
            words_out.at[piece], words_in.at[piece], word_send.at[piece], word_recv.at[piece],
            device_id=owner(o), device_id_type=MESH,
        )

    far = range(chips - 1, 3, -1)
    order = [chip ^ o for o in (3, *far, 1, 2, 0)]
    strip_copy = pltpu.make_async_copy(strip_hbm, strip, strip_sem)
    strip_copy.start()
    for g in order:
        staged(g).start()
        mine(g).start()

    barrier = pltpu.get_barrier_semaphore()
    for o in range(1, peers + 1):
        pl.semaphore_signal(barrier, inc=1, device_id=peer(o), device_id_type=MESH)
    for o in range(1, chips):
        pl.semaphore_signal(barrier, inc=1, device_id=owner(o), device_id_type=MESH)
    strip_copy.wait()
    for i in range(width // TILE):
        start = width - TILE - i * TILE
        table[pl.ds(i * TILE, TILE), :] = strip[:, start : start + width]
    sums[:, :, last:] = jnp.zeros((3, owned, TILE), jnp.float32)
    pl.semaphore_wait(barrier, peers + chips - 1)

    mask_copy = pltpu.make_async_remote_copy(
        mask_ref, mask_in, mask_send, mask_recv, device_id=partner, device_id_type=MESH
    )
    mask_copy.start()
    for g in order:
        staged(g).wait()
        swapped(g).start()
    mask_copy.wait_recv()
    both_masks = jnp.concatenate([mask_ref[...], mask_in[...]], axis=0).astype(jnp.float32)
    mask_turned[...] = both_masks.T

    def mask_rows(block, count):
        rows = mask_turned[pl.ds(pl.multiple_of(block * owned, owned), owned), :]
        return jnp.concatenate([rows[:, d : d + 1] for d in range(count)], axis=0)

    def statistics(step, carry):
        g = chip ^ (chips - 1 - step)
        mine(g).wait()
        of_pairs = mask_rows(2 * g + core, all_days)
        row_mask[g] = of_pairs.reshape(all_days, owned, 1)
        for x_ref, rows in ((rows_ref.at[g, pl.ds(0, days)], of_pairs[: days * owned]),
                            (stage.at[g], mask_rows(2 * g + 1 - core, days))):
            x = x_ref[...].reshape(days * owned, lag_count).astype(jnp.float32)
            energy = jnp.sum(x * x, axis=1, keepdims=True) * rows
            both = jnp.concatenate(
                [jnp.broadcast_to(energy, (days * owned, 128)), jnp.broadcast_to(rows, (days * owned, 128))], axis=1
            )
            carry = carry + jnp.sum(both.reshape(days, owned, 256), axis=1)
        return carry

    found = lax.fori_loop(0, chips, statistics, jnp.zeros((days, 256), jnp.float32))
    none = jnp.zeros_like(found)
    stat_out[...] = jnp.where(
        core == 0, jnp.concatenate([found, none], axis=0), jnp.concatenate([none, found], axis=0)
    )
    for o in range(1, peers + 1):
        told(o).start()

    def transform(g, here, cols):
        lhs = rows_ref[g, :, here, :].reshape(-1, lag_count)
        return jnp.dot(lhs, table[:lag_count, cols], preferred_element_type=jnp.float32)

    def add_days(g, here, cols, hilbert):
        size = cols.stop - cols.start
        count = hilbert.shape[0] // all_days
        scale = (day_weight[:, :count] * row_mask[g, :, here, :]).reshape(-1, 1)
        real = scale * rows_ref[g, :, here, cols].reshape(-1, size).astype(jnp.float32)
        imag = scale * hilbert
        inverse = lax.rsqrt(real * real + imag * imag + 0.25)
        for k, term in enumerate((real, real * inverse, imag * inverse)):
            sums[k, :count, cols] = jnp.sum(term.reshape(all_days, count, size), axis=0)

    def encode(piece, rows, o):
        linear, linear_units = codes(sums[0, rows])
        first, first_units = codes(sums[1, rows])
        second, second_units = codes(sums[2, rows])
        words_out[piece, :, :width] = join(first, second)
        words_out[piece, :, width : width + half] = join(linear[:, :half], linear[:, half:])
        pick = lax.broadcasted_iota(jnp.int32, (part, 128), 1)
        words_out[piece, :, width + half :] = jnp.where(
            pick == 0, linear_units, jnp.where(pick == 1, first_units, second_units)
        )
        shipped(piece, o).start()

    def decode(piece, rows):
        units = words_in[piece, :, width + half :].astype(jnp.float32) * (1.0 / (FULL * UNIT))
        left, right = split(words_in[piece, :, width : width + half])
        sums[0, rows, :half] += left.astype(jnp.float32) * units[:, 0:1]
        sums[0, rows, half:] += right.astype(jnp.float32) * units[:, 0:1]
        first, second = split(words_in[piece, :, :width])
        sums[1, rows] += first.astype(jnp.float32) * units[:, 1:2]
        sums[2, rows] += second.astype(jnp.float32) * units[:, 2:3]

    whole, low, high = pl.ds(0, owned), pl.ds(0, part), pl.ds(part, part)

    swapped(order[0]).wait_recv()
    for cols in tiles:
        first_hilbert[:, cols] = transform(order[0], whole, cols)

    for o in range(1, peers + 1):
        told(o).wait_recv()
    stats = stat_out[...]
    for o in range(peers):
        stats = stats + stat_in[o]
    weight = lax.rsqrt(stats[:, :128] / (lag_count * jnp.maximum(stats[:, 128:], 1.0)) + 0.1)
    weight = jnp.where(core == 0, weight, jnp.concatenate([weight[days:], weight[:days]], axis=0))
    for d in range(all_days):
        day_weight[d] = jnp.broadcast_to(weight[d : d + 1, :1], (owned, 1))

    for cols in tiles:
        add_days(order[0], whole, cols, first_hilbert[:, cols])
    encode(0, low, 1)
    encode(1, high, 2)

    def far_block(step, carry):
        o = chips - 1 - step
        swapped(chip ^ o).wait_recv()
        for cols in tiles:
            add_days(chip ^ o, whole, cols, transform(chip ^ o, whole, cols))
        encode(2 * o - 2, low, o)
        encode(2 * o - 1, high, o)
        return carry

    if chips > 4:
        lax.fori_loop(0, chips - 4, far_block, 0)

    def near_half(q, carry):
        o = 1 + q % 2
        g = chip ^ o
        here = pl.ds(pl.multiple_of(((q + q // 2) % 2) * part, part), part)

        @pl.when(q < 2)
        def _():
            swapped(g).wait_recv()

        for cols in tiles:
            add_days(g, here, cols, transform(g, here, cols))

        @pl.when(q >= 2)
        def _():
            shipped(3 - q, o).wait_recv()
            decode(3 - q, low)

        encode(2 + q, low, o)
        return carry

    lax.fori_loop(0, 4, near_half, 0)
    swapped(chip).wait_recv()
    for cols in tiles:
        add_days(chip, whole, cols, transform(chip, whole, cols))

    def arrive(piece, carry):
        turn = piece + jnp.where(piece // 2 == 2, 1, 0)
        shipped(piece, 1).wait_recv()
        decode(piece, pl.ds(pl.multiple_of((turn % 2) * part, part), part))
        return carry

    lax.fori_loop(2, pieces, arrive, 0)
    real, imag = sums[1, :, :lag_count], sums[2, :, :lag_count]
    linear_ref[...] = sums[0, :, :lag_count]
    power_ref[...] = real * real + imag * imag

    mask_copy.wait_send()
    for g in range(chips):
        swapped(g).wait_send()
    for o in range(1, peers + 1):
        told(o).wait_send()
    for piece in range(pieces):
        shipped(piece, 1).wait_send()


def general_sums(correlations, mask):
    days, pairs, lag_count = correlations.shape
    groups = lax.axis_size("day")
    chips = groups // 2
    owned = pairs // groups
    width = padded(lag_count)
    peers = 2 * lax.axis_size("pair") - 1

    strip = jnp.asarray(kernel_strip(lag_count))
    size = width + width // 2 + 128
    pieces = 2 * chips - 2
    out = jax.ShapeDtypeStruct((owned, lag_count), jnp.float32)
    vmem = pl.BlockSpec(memory_space=pltpu.VMEM)
    hbm = pl.BlockSpec(memory_space=pl.ANY)
    dma = pltpu.SemaphoreType.DMA
    return pl.pallas_call(
        functools.partial(stack_kernel, lag_count),
        in_specs=[hbm, vmem, hbm],
        out_specs=(vmem, vmem),
        out_shape=(out, out),
        scratch_shapes=[
            pltpu.VMEM((chips, 2 * days, owned, lag_count), jnp.bfloat16),
            pltpu.VMEM((chips, days, owned, lag_count), jnp.bfloat16),
            pltpu.VMEM(strip.shape, jnp.bfloat16),
            pltpu.VMEM((width, width), jnp.bfloat16),
            pltpu.VMEM((3, owned, width), jnp.float32),
            pltpu.VMEM((2 * days * owned, width), jnp.float32),
            pltpu.VMEM((days, pairs), jnp.int32),
            pltpu.VMEM((pairs, 2 * days), jnp.float32),
            pltpu.VMEM((chips, 2 * days, owned, 1), jnp.float32),
            pltpu.VMEM((2 * days, owned, 1), jnp.float32),
            pltpu.VMEM((2 * days, 256), jnp.float32),
            pltpu.VMEM((peers, 2 * days, 256), jnp.float32),
            pltpu.VMEM((pieces, owned // 2, size), jnp.int32),
            pltpu.VMEM((pieces, owned // 2, size), jnp.int32),
            dma((chips,)), dma((chips,)), dma, dma((chips,)), dma((chips,)), dma, dma,
            dma((peers,)), dma((peers,)), dma((pieces,)), dma((pieces,)),
        ],
        compiler_params=pltpu.CompilerParams(
            vmem_limit_bytes=46 * 2**20, collective_id=0, has_side_effects=True
        ),
        name="stack",
    )(correlations.reshape(days, groups, owned, lag_count), mask, strip)


LANES = 128
CHUNK = 512
HALF = CHUNK // 2
ROWS = HALF // 2
WORDS = ROWS + ROWS // 2
PACK = WORDS + 8
SENT = WORDS + 3


def block_strip(lag_count):
    f32 = np.float32
    offset = np.arange(lag_count, dtype=np.int32)
    offset = np.where(offset > lag_count // 2, offset - lag_count, offset)
    angle = f32(np.pi) * offset.astype(f32) / f32(lag_count)
    parity = f32(1) - f32(2) * (offset % 2).astype(f32)
    sine = np.where(offset == 0, f32(1), np.sin(angle)).astype(f32)
    kernel = np.where(offset == 0, f32(0), (np.cos(angle) - parity) / (f32(lag_count) * sine))
    width = chunked(lag_count)
    index = np.arange(TILE)[:, None] - np.arange(2 * width - TILE)[None, :] + (width - TILE)
    return kernel.astype(f32)[index % lag_count].astype(jnp.bfloat16)


def chunked(lag_count):
    return -(-lag_count // CHUNK) * CHUNK


def sorting_matrix(rows):
    lags = TILE // rows
    out = np.arange(TILE)
    source = (out % lags) * rows + out // lags
    return (source[:, None] == np.arange(TILE)[None, :]).astype(jnp.bfloat16)


def fast_kernel(
    lag_count, x_hbm, mask_hbm, counts_hbm, strip_hbm, sorter_hbm, power_ref, linear_ref, inverse_ref,
    mask_ref, counts_ref, sorter, raw, own, theirs, strip, even_h, odd_h, sums, scale, bias, mask_in, stat_out, stat_in,
    coded, parts, partial_in, relay_out, final_in, total,
    load_sem, small_sem, swap_send, swap_recv, late_send, late_recv, mask_send, mask_recv, stat_send, stat_recv,
    partial_send, partial_recv, final_send, final_recv, own_send, own_recv,
):
    f32 = jnp.float32
    width = raw.shape[0]
    planes = raw.shape[1]
    loads = width // TILE
    chunks = width // CHUNK
    steps = 2 * chunks
    peers = stat_in.shape[0]
    days = mask_ref.shape[0]
    tiles = mask_ref.shape[1] // LANES
    lags = TILE // planes
    me, plane = lax.axis_index("day"), lax.axis_index("pair")
    chip, core = me // 2, me % 2
    partner = {"day": me ^ 1, "pair": plane}

    def pick(s, table):
        return sum(jnp.where(s == i, value, 0) for i, value in enumerate(table))

    def order(s):
        return (
            jnp.where(core == 0, pick(s, (0, 0, 0, 1, 0, 1, 1, 1)), s // chunks),
            jnp.where(core == 0, pick(s, (0, 1, 2, 0, 3, 1, 2, 3)), pick(s, (3, 2, 1, 0, 0, 1, 2, 3))),
        )

    def near_step(k):
        return jnp.where(core == 0, pick(k, (3, 5, 6, 7)), pick(k, (3, 2, 1, 0)))

    def route(k, half):
        return pick(2 * k + half, (0, 0, 0, 1, 0, 1, 1, 1)), pick(2 * k + half, (0, 1, 2, 0, 3, 1, 2, 3))

    def near(o, c):
        return {"day": 2 * (chip ^ o) + c, "pair": plane}

    def peer(o):
        rank = (2 * plane + core + o) % (peers + 1)
        return {"day": 2 * chip + rank % 2, "pair": rank // 2}

    def loaded(j, count=TILE):
        rows = pl.ds(j * TILE, count)
        return pltpu.make_async_copy(x_hbm.at[rows], raw.at[rows], load_sem.at[j])

    def remote(source, target, send, recv, device):
        return pltpu.make_async_remote_copy(
            source, target, send, recv, device_id=device, device_id_type=MESH
        )

    def mine(slot):
        return 2 * (1 - core) + 1 - slot

    def swapped(j):
        rows = pl.ds(pl.multiple_of(j * TILE, TILE), TILE)
        return remote(
            own.at[2 * core + 1, :, rows], theirs.at[0, :, rows], swap_send.at[j], swap_recv.at[j], partner
        )

    def swapped_late():
        return remote(own.at[2 * core], theirs.at[1], late_send, late_recv, partner)

    def told(o):
        return remote(stat_out, stat_in.at[o - 1], stat_send.at[o - 1], stat_recv.at[o - 1], peer(o))

    sent = pl.ds(0, SENT)

    def relayed(s, k, half):
        far, j = route(k, half)
        return remote(
            coded.at[s, half, :, sent], partial_in.at[j, :, sent], partial_send.at[k, half], partial_recv.at[j],
            near(2 - far, 1 - far),
        )

    def finished(source, k, half, c):
        return remote(
            source.at[sent], final_in.at[1 - core, k, half, sent], final_send.at[k, half, c],
            final_recv.at[1 - core, k, half], near(2 - core, c),
        )

    def handed(s, k, half):
        return remote(
            parts.at[s, half, 0], total.at[k, half], own_send.at[k, half], own_recv.at[k, half], partner
        )

    last = loads - 1
    small = [
        pltpu.make_async_copy(source, target, small_sem.at[i])
        for i, (source, target) in enumerate(
            ((sorter_hbm, sorter), (mask_hbm, mask_ref), (counts_hbm, counts_ref), (strip_hbm, strip))
        )
    ]
    for copy in small[:3]:
        copy.start()
    for j in range(last):
        loaded(j).start()
    loaded(last, lag_count - last * TILE).start()
    small[3].start()
    barrier = pltpu.get_barrier_semaphore()
    for o in range(1, peers + 1):
        pl.semaphore_signal(barrier, inc=1, device_id=peer(o), device_id_type=MESH)
    for o in (1, 2):
        for c in (0, 1):
            pl.semaphore_signal(barrier, inc=1, device_id=near(o, c), device_id_type=MESH)
    raw[lag_count:] = jnp.zeros((width - lag_count, planes, LANES), raw.dtype)
    pl.semaphore_wait(barrier, peers + 4)
    small[0].wait()
    small[1].wait()
    mask_copy = remote(mask_ref, mask_in, mask_send, mask_recv, partner)
    mask_copy.start()

    def sort(j, energy):
        energy = [energy[i] for i in range(planes)]
        for g in range(TILE // (2 * lags)):
            at = pl.multiple_of(j * TILE + g * 2 * lags, 2 * lags)
            pair = [raw[pl.ds(at + h * lags, lags)].reshape(TILE, LANES) for h in (0, 1)]
            out = jnp.dot(sorter[...], jnp.concatenate(pair, axis=1), preferred_element_type=f32)
            for t in range(tiles):
                for d in range(days):
                    i = t * days + d
                    lane = (d % 2) * LANES
                    for h in (0, 1):
                        value = out[i * lags : (i + 1) * lags, h * LANES : (h + 1) * LANES]
                        energy[i] = energy[i] + jnp.sum((value * value).reshape(-1, 8, LANES), axis=0)
                        own[chip ^ t, d // 2, pl.ds(at + h * lags, lags), lane : lane + LANES] = value.astype(own.dtype)
        return jnp.stack(energy)

    def sort_load(j, energy):
        loaded(j).wait()
        energy = sort(j, energy)
        swapped(j).start()
        return energy

    energy = lax.fori_loop(0, last, sort_load, jnp.zeros((planes, 8, LANES), f32))
    loaded(last, lag_count - last * TILE).wait()
    energy = sort(last, energy)
    swapped(last).start()
    swapped_late().start()

    found, used = [], []
    for d in range(days):
        rows = [mask_ref[d : d + 1, t * LANES : (t + 1) * LANES].astype(f32) for t in range(tiles)]
        one = sum(jnp.sum(energy[t * days + d], axis=0, keepdims=True) * rows[t] for t in range(tiles))
        found.append(one)
        used.append(sum(rows))
    stat_out[...] = jnp.concatenate(found + used, axis=0)
    for o in range(1, peers + 1):
        told(o).start()

    def operand(slot, dp):
        return own[mine(slot), dp] if dp < days // 2 else theirs[slot, dp - days // 2]

    parts_of = CHUNK // TILE

    def transform_piece(slot, k, piece, target):
        dp, part = piece // parts_of, piece % parts_of
        start = pl.multiple_of(width - TILE - (k * parts_of + part) * TILE, TILE)
        target[part * TILE : (part + 1) * TILE, dp * TILE : (dp + 1) * TILE] = jnp.dot(
            strip[:, pl.ds(start, width)], operand(slot, dp), preferred_element_type=f32
        )

    def transform(slot, k, pieces, target):
        for piece in pieces:
            transform_piece(slot, k, piece, target)

    def add_days(slot, k, first, stop, source):
        size = 32
        for row in range(first, stop, size):
            at = pl.multiple_of(k * CHUNK + row, size)
            lin = one = two = jnp.zeros((size // 8, 8, LANES), f32)
            for e in range(2 * days):
                dp, lane = e // 2, (e % 2) * LANES
                if e < days:
                    x = own[mine(slot), dp, pl.ds(at, size), lane : lane + LANES]
                else:
                    x = theirs[slot, dp - days // 2, pl.ds(at, size), lane : lane + LANES]
                x = x.astype(f32).reshape(size // 8, 8, LANES)
                h = source[row : row + size, e * LANES : (e + 1) * LANES].reshape(size // 8, 8, LANES)
                r = lax.rsqrt(x * x + h * h + bias[slot, e][None])
                lin = lin + x * scale[slot, e][None]
                one = one + x * r
                two = two + h * r
            for v, value in enumerate((lin, one, two)):
                sums[v, row : row + size] = value.reshape(size, LANES)

    low_lane = lax.broadcasted_iota(jnp.int32, (ROWS, LANES), 1) < LANES // 2

    def split(half, v, c):
        a = sums[v, half * HALF : half * HALF + ROWS]
        b = sums[v, half * HALF + ROWS : (half + 1) * HALF]
        if c == 0:
            return jnp.where(low_lane, a, pltpu.roll(b, LANES // 2, 1))
        return jnp.where(low_lane, pltpu.roll(a, LANES // 2, 1), b)

    def encode(target, values):
        codes_of, units = [], []
        for value in values:
            top = jnp.max(jnp.abs(value), axis=0, keepdims=True)
            unit = (top * UNIT).astype(jnp.int32) + 1
            step = FULL * UNIT / unit.astype(f32)
            codes_of.append((value * step + 32768.5).astype(jnp.int32))
            units.append(unit)
        lin, one, two = codes_of
        target[:ROWS] = one * 65536 + two
        target[ROWS:WORDS] = lin[: ROWS // 2] * 65536 + lin[ROWS // 2 :]
        pick = lax.broadcasted_iota(jnp.int32, (8, LANES), 0)
        target[WORDS:] = jnp.where(pick == 0, units[0], jnp.where(pick == 1, units[1], units[2]))

    def decode(source):
        units = source[WORDS:].astype(f32) * (1.0 / (FULL * UNIT))

        def value(code, v):
            return (code.astype(f32) - 32768.0) * units[v : v + 1]

        def pieces(word):
            return lax.shift_right_logical(word, jnp.full_like(word, 16)), word & 65535

        one, two = pieces(source[:ROWS])
        top, bottom = pieces(source[ROWS:WORDS])
        return (jnp.concatenate([value(top, 0), value(bottom, 0)], axis=0), value(one, 1), value(two, 2))

    def code(s, half, c):
        values = [split(half, v, c) for v in range(3)]
        for v in range(3):
            parts[s, half, c, v] = values[v]
        encode(coded.at[s, half, c], values)

    def step_both(s, source, target):
        slot, k = order(s)
        rows = (0, 96, 192, 288, 384, 448, CHUNK)
        for piece in range(2 * days):
            if piece < len(rows) - 1:
                add_days(slot, k, rows[piece], rows[piece + 1], source)
            if piece in (3, 4):
                code(s, 0, piece - 3)
            if piece in (6, 7):
                code(s, 1, piece - 6)
            if target is not None:
                transform_piece(*order(s + 1), piece, target)

    def send(s, halves=(0, 1)):
        slot, k = order(s)

        for half in halves:
            @pl.when(jnp.logical_and(slot + core == 1, route(k, half)[0] == core))
            def _():
                for c in (0, 1):
                    finished(coded.at[s, half, c], k, half, c).start()

        @pl.when(slot + core == 0)
        def _():
            for half in halves:
                relayed(s, k, half).start()

        @pl.when(slot + core == 2)
        def _():
            for half in halves:
                handed(s, k, half).start()

    def relay(j):
        k = jnp.where(core == 0, pick(j, (1, 2, 3, 3)), pick(j, (0, 0, 1, 2)))
        half = jnp.where(core == 0, pick(j, (1, 1, 0, 1)), pick(j, (0, 1, 0, 0)))
        s = near_step(k)
        remote(
            coded.at[0, 0, :, sent], partial_in.at[j, :, sent], partial_send.at[0, 0], partial_recv.at[j], partner
        ).wait_recv()
        for c in (0, 1):
            far = decode(partial_in.at[j, c])
            encode(relay_out.at[j, c], [parts[s, half, c, v] + far[v] for v in range(3)])
            finished(relay_out.at[j, c], k, half, c).start()

    small[3].wait()
    transform(*order(0), range(days), even_h)
    for j in range(loads):
        swapped(j).wait_recv()
    transform(*order(0), range(days, 2 * days), even_h)
    transform(*order(1), range(2 * days), odd_h)

    mask_copy.wait_recv()
    for o in range(1, peers + 1):
        told(o).wait_recv()
    ours, other = stat_out[...], jnp.zeros_like(stat_out)
    for o in range(1, peers + 1):
        if o % 2:
            other = other + stat_in[o - 1]
        else:
            ours = ours + stat_in[o - 1]
    for which, stats in enumerate((ours, other)):
        row = jnp.sum(stats, axis=1, keepdims=True)
        power = row[:days] / (lag_count * jnp.maximum(row[days:], 1.0)) + 0.1
        weight = lax.rsqrt(power)
        for slot in (0, 1):
            at = pl.multiple_of((chip ^ mine(slot)) * LANES, LANES)
            usable = (mask_in if which else mask_ref)[:, pl.ds(at, LANES)].astype(f32)
            by_day = weight * usable
            offset = jnp.where(usable > 0.0, 0.25 * power, jnp.inf)
            for d in range(days):
                scale[slot, which * days + d] = jnp.broadcast_to(by_day[d : d + 1], (8, LANES))
                bias[slot, which * days + d] = jnp.broadcast_to(offset[d : d + 1], (8, LANES))
    for half in (0, 1):
        add_days(*order(0), half * HALF, half * HALF + HALF, even_h)
        code(0, half, 0)
        code(0, half, 1)
        send(0, (half,))
    swapped_late().wait_recv()

    def step(i, carry):
        for s, target, source in ((2 * i + 1, even_h, odd_h), (2 * i + 2, odd_h, even_h)):
            step_both(s, source, target)
            send(s)
            if source is odd_h:
                @pl.when(jnp.logical_and(core == 1, i == 1))
                def _():
                    lax.fori_loop(0, 2, lambda j, carry: (relay(j), carry)[1], 0)

                @pl.when(i == 2)
                def _():
                    relay(3 * core)
            else:
                @pl.when(i + core == 2)
                def _():
                    relay(1 + core)
        return carry

    lax.fori_loop(0, chunks - 1, step, 0)
    step_both(steps - 1, odd_h, None)
    send(steps - 1)

    @pl.when(core == 0)
    def _():
        lax.fori_loop(2, chunks, lambda j, carry: (relay(j), carry)[1], 0)

    small[2].wait()
    inverse_ref[...] = 1.0 / jnp.maximum(counts_ref[...].astype(f32), 1.0)

    @pl.when(core == 0)
    def _():
        for k in range(chunks):
            for half in (0, 1):
                handed(0, k, half).wait_recv()

    @pl.when(core == 1)
    def _():
        def keep(k, carry):
            for half in (0, 1):
                for v in range(3):
                    total[k, half, v] = parts[chunks + k, half, 1, v]
            return carry

        lax.fori_loop(0, chunks, keep, 0)

    def settle():
        mask_copy.wait_send()
        swapped_late().wait_send()
        for j in range(loads):
            swapped(j).wait_send()
        for o in range(1, peers + 1):
            told(o).wait_send()
        for k in range(chunks):
            for half in (0, 1):
                for c in (0, 1):
                    finished(relay_out.at[0, 0], k, half, c).wait_send()

            @pl.when(core == 0)
            def _():
                for half in (0, 1):
                    relayed(0, k, half).wait_send()

            @pl.when(core == 1)
            def _():
                for half in (0, 1):
                    handed(0, k, half).wait_send()

    seen = set()
    arrivals = (
        (0, 3, 0), (0, 3, 1), (0, 2, 1), (0, 1, 1), (1, 0, 0), (1, 0, 1), (0, 0, 0), (0, 0, 1),
        (1, 1, 0), (0, 1, 0), (1, 1, 1), (0, 2, 0), (1, 2, 0), (1, 2, 1), (1, 3, 0), (1, 3, 1),
    )
    for s, k, half in arrivals:
        if (s, k, half) == (1, 3, 0):
            settle()
        remote(
            relay_out.at[0, 0, sent], final_in.at[s, k, half, sent], final_send.at[k, half, 0],
            final_recv.at[s, k, half], partner,
        ).wait_recv()
        found = decode(final_in.at[s, k, half])
        if (k, half) not in seen:
            seen.add((k, half))
            for v in range(3):
                total[k, half, v] += found[v]
            continue
        lin, one, two = (total[k, half, v] + found[v] for v in range(3))
        for ref, value in ((linear_ref, lin), (power_ref, one * one + two * two)):
            turned = value.T
            for part in (0, 1):
                start = k * CHUNK + half * HALF + part * ROWS
                stop = min(start + ROWS, lag_count)
                if stop > start:
                    rows = turned[part * LANES // 2 : (part + 1) * LANES // 2]
                    ref[:, start:stop] = rows[:, : stop - start]


def fast_stack(correlations, mask, counts):
    days, pairs, lag_count = correlations.shape
    owned = pairs // lax.axis_size("day")
    peers = 2 * lax.axis_size("pair") - 1
    tiles = pairs // LANES
    planes = tiles * days
    width = chunked(lag_count)
    chunks, loads = width // CHUNK, width // TILE
    by_lag = correlations.transpose(2, 0, 1).reshape(lag_count, days, tiles, LANES)
    by_lag = by_lag.transpose(0, 2, 1, 3).reshape(lag_count, planes, LANES)
    strip = jnp.asarray(block_strip(lag_count))
    sorter = jnp.asarray(sorting_matrix(planes))
    out = jax.ShapeDtypeStruct((owned, lag_count), jnp.float32)
    vmem = pl.BlockSpec(memory_space=pltpu.VMEM)
    hbm = pl.BlockSpec(memory_space=pltpu.HBM)
    dma = pltpu.SemaphoreType.DMA
    bf16, f32, i32 = jnp.bfloat16, jnp.float32, jnp.int32
    power, linear_sum, inverse = pl.pallas_call(
        functools.partial(fast_kernel, lag_count),
        in_specs=[hbm] * 5,
        out_specs=(vmem, vmem, vmem),
        out_shape=(out, out, jax.ShapeDtypeStruct((1, owned), f32)),
        scratch_shapes=[
            pltpu.VMEM(mask.shape, i32),
            pltpu.VMEM((1, owned), i32),
            pltpu.VMEM(sorter.shape, bf16),
            pltpu.VMEM((width, planes, LANES), bf16),
            pltpu.VMEM((tiles, days // 2, width, TILE), bf16),
            pltpu.VMEM((2, days // 2, width, TILE), bf16),
            pltpu.VMEM(strip.shape, bf16),
            pltpu.VMEM((CHUNK, 2 * days * LANES), f32),
            pltpu.VMEM((CHUNK, 2 * days * LANES), f32),
            pltpu.VMEM((3, CHUNK, LANES), f32),
            pltpu.VMEM((2, 2 * days, 8, LANES), f32),
            pltpu.VMEM((2, 2 * days, 8, LANES), f32),
            pltpu.VMEM(mask.shape, i32),
            pltpu.VMEM((2 * days, LANES), f32),
            pltpu.VMEM((peers, 2 * days, LANES), f32),
            pltpu.VMEM((2 * chunks, 2, 2, PACK, LANES), i32),
            pltpu.VMEM((2 * chunks, 2, 2, 3, ROWS, LANES), f32),
            pltpu.VMEM((chunks, 2, PACK, LANES), i32),
            pltpu.VMEM((chunks, 2, PACK, LANES), i32),
            pltpu.VMEM((2, chunks, 2, PACK, LANES), i32),
            pltpu.VMEM((chunks, 2, 3, ROWS, LANES), f32),
            dma((loads,)), dma((4,)), dma((loads,)), dma((loads,)), dma, dma, dma, dma, dma((peers,)), dma((peers,)),
            dma((chunks, 2)), dma((chunks,)), dma((chunks, 2, 2)), dma((2, chunks, 2)),
            dma((chunks, 2)), dma((chunks, 2)),
        ],
        compiler_params=pltpu.CompilerParams(
            vmem_limit_bytes=46 * 2**20, collective_id=0, has_side_effects=True
        ),
        name="stack",
    )(*(pltpu.with_memory_space_constraint(v, pltpu.HBM) for v in (by_lag, mask, counts.reshape(1, owned), strip, sorter)))
    return linear_sum, power, inverse.reshape(owned, 1)


def shards(correlations, mask, counts):
    days, pairs, lag_count = correlations.shape
    groups = lax.axis_size("day")
    four = groups == 8 and days == 4 and chunked(lag_count) == 4 * CHUNK
    if four and pairs == 4 * LANES:
        linear_sum, power, inverse = fast_stack(correlations, mask, counts)
    else:
        linear_sum, power = general_sums(correlations, mask)
        inverse = (1.0 / jnp.maximum(counts.astype(jnp.float32), 1.0))[:, None]
    linear = linear_sum * inverse
    return (linear * (power * (inverse * inverse)), linear)


def solution(mesh):
    placed = (P("day", "pair", None), P("day", "pair"), P(("pair", "day")))
    return jax.shard_map(
        shards,
        mesh=mesh,
        in_specs=placed,
        out_specs=(P(("pair", "day"), None), P(("pair", "day"), None)),
        check_vma=False,
    )
```

```python
import functools

import jax
import jax.numpy as jnp
import numpy as np
from jax import lax
from jax.experimental import pallas as pl
from jax.experimental.pallas import tpu as pltpu
from jax.sharding import PartitionSpec as P

TILE = 256
MESH = pl.DeviceIdType.MESH
FULL = 32767.0
UNIT = 2.0**20


def padded(lag_count):
    return -(-lag_count // TILE) * TILE


def kernel_strip(lag_count):
    f32 = np.float32
    offset = np.arange(lag_count, dtype=np.int32)
    offset = np.where(offset > lag_count // 2, offset - lag_count, offset)
    angle = f32(np.pi) * offset.astype(f32) / f32(lag_count)
    parity = f32(1) - f32(2) * (offset % 2).astype(f32)
    sine = np.where(offset == 0, f32(1), np.sin(angle)).astype(f32)
    kernel = np.where(offset == 0, f32(0), (np.cos(angle) - parity) / (f32(lag_count) * sine))
    width = padded(lag_count)
    index = np.arange(2 * width - TILE)[None, :] - np.arange(TILE)[:, None] - (width - TILE)
    return kernel.astype(f32)[index % lag_count].astype(jnp.bfloat16)


def codes(values):
    top = jnp.max(jnp.abs(values), axis=1, keepdims=True)
    units = (top * UNIT).astype(jnp.int32) + 1
    step = FULL * UNIT / units.astype(jnp.float32)
    return jnp.round(values * step).astype(jnp.int32), units


def join(high, low):
    return high * 65536 + (low & 65535)


def split(word):
    low = ((word & 65535) ^ 32768) - 32768
    return word >> 16, low


def stack_kernel(
    lag_count, x_hbm, mask_ref, strip_hbm, linear_ref, power_ref,
    rows_ref, stage, strip, table, sums, first_hilbert, mask_in, mask_turned, row_mask, day_weight,
    stat_out, stat_in, words_out, words_in,
    load_sem, stage_sem, strip_sem, swap_send, swap_recv, mask_send, mask_recv,
    stat_send, stat_recv, word_send, word_recv,
):
    width = table.shape[1]
    half = width // 2
    chips, all_days, owned, _ = rows_ref.shape
    days = all_days // 2
    total = all_days * owned
    part = owned // 2
    pieces = words_out.shape[0]
    peers = stat_in.shape[0]
    me, plane = lax.axis_index("day"), lax.axis_index("pair")
    chip, core = me // 2, me % 2
    partner = {"day": me ^ 1, "pair": plane}
    last = width - TILE
    tiles = [slice(j * TILE, min((j + 1) * TILE, lag_count)) for j in range(width // TILE)]

    def mine(g):
        return pltpu.make_async_copy(x_hbm.at[:, 2 * g + core], rows_ref.at[g, pl.ds(0, days)], load_sem.at[g])

    def staged(g):
        return pltpu.make_async_copy(x_hbm.at[:, 2 * g + 1 - core], stage.at[g], stage_sem.at[g])

    def swapped(g):
        return pltpu.make_async_remote_copy(
            stage.at[g], rows_ref.at[g, pl.ds(days, days)], swap_send.at[g], swap_recv.at[g],
            device_id=partner, device_id_type=MESH,
        )

    def peer(o):
        rank = (2 * plane + core + o) % (peers + 1)
        return {"day": 2 * chip + rank % 2, "pair": rank // 2}

    def told(o):
        return pltpu.make_async_remote_copy(
            stat_out, stat_in.at[o - 1], stat_send.at[o - 1], stat_recv.at[o - 1],
            device_id=peer(o), device_id_type=MESH,
        )

    def owner(o):
        return {"day": 2 * (chip ^ o) + core, "pair": plane}

    def shipped(piece, o):
        return pltpu.make_async_remote_copy(
            words_out.at[piece], words_in.at[piece], word_send.at[piece], word_recv.at[piece],
            device_id=owner(o), device_id_type=MESH,
        )

    far = range(chips - 1, 3, -1)
    order = [chip ^ o for o in (3, *far, 1, 2, 0)]
    strip_copy = pltpu.make_async_copy(strip_hbm, strip, strip_sem)
    strip_copy.start()
    for g in order:
        staged(g).start()
        mine(g).start()

    barrier = pltpu.get_barrier_semaphore()
    for o in range(1, peers + 1):
        pl.semaphore_signal(barrier, inc=1, device_id=peer(o), device_id_type=MESH)
    for o in range(1, chips):
        pl.semaphore_signal(barrier, inc=1, device_id=owner(o), device_id_type=MESH)
    strip_copy.wait()
    for i in range(width // TILE):
        start = width - TILE - i * TILE
        table[pl.ds(i * TILE, TILE), :] = strip[:, start : start + width]
    sums[:, :, last:] = jnp.zeros((3, owned, TILE), jnp.float32)
    pl.semaphore_wait(barrier, peers + chips - 1)

    mask_copy = pltpu.make_async_remote_copy(
        mask_ref, mask_in, mask_send, mask_recv, device_id=partner, device_id_type=MESH
    )
    mask_copy.start()
    for g in order:
        staged(g).wait()
        swapped(g).start()
    mask_copy.wait_recv()
    both_masks = jnp.concatenate([mask_ref[...], mask_in[...]], axis=0).astype(jnp.float32)
    mask_turned[...] = both_masks.T

    def mask_rows(block, count):
        rows = mask_turned[pl.ds(pl.multiple_of(block * owned, owned), owned), :]
        return jnp.concatenate([rows[:, d : d + 1] for d in range(count)], axis=0)

    def statistics(step, carry):
        g = chip ^ (chips - 1 - step)
        mine(g).wait()
        of_pairs = mask_rows(2 * g + core, all_days)
        row_mask[g] = of_pairs.reshape(all_days, owned, 1)
        for x_ref, rows in ((rows_ref.at[g, pl.ds(0, days)], of_pairs[: days * owned]),
                            (stage.at[g], mask_rows(2 * g + 1 - core, days))):
            x = x_ref[...].reshape(days * owned, lag_count).astype(jnp.float32)
            energy = jnp.sum(x * x, axis=1, keepdims=True) * rows
            both = jnp.concatenate(
                [jnp.broadcast_to(energy, (days * owned, 128)), jnp.broadcast_to(rows, (days * owned, 128))], axis=1
            )
            carry = carry + jnp.sum(both.reshape(days, owned, 256), axis=1)
        return carry

    found = lax.fori_loop(0, chips, statistics, jnp.zeros((days, 256), jnp.float32))
    none = jnp.zeros_like(found)
    stat_out[...] = jnp.where(
        core == 0, jnp.concatenate([found, none], axis=0), jnp.concatenate([none, found], axis=0)
    )
    for o in range(1, peers + 1):
        told(o).start()

    def transform(g, here, cols):
        lhs = rows_ref[g, :, here, :].reshape(-1, lag_count)
        return jnp.dot(lhs, table[:lag_count, cols], preferred_element_type=jnp.float32)

    def add_days(g, here, cols, hilbert):
        size = cols.stop - cols.start
        count = hilbert.shape[0] // all_days
        scale = (day_weight[:, :count] * row_mask[g, :, here, :]).reshape(-1, 1)
        real = scale * rows_ref[g, :, here, cols].reshape(-1, size).astype(jnp.float32)
        imag = scale * hilbert
        inverse = lax.rsqrt(real * real + imag * imag + 0.25)
        for k, term in enumerate((real, real * inverse, imag * inverse)):
            sums[k, :count, cols] = jnp.sum(term.reshape(all_days, count, size), axis=0)

    def encode(piece, rows, o):
        linear, linear_units = codes(sums[0, rows])
        first, first_units = codes(sums[1, rows])
        second, second_units = codes(sums[2, rows])
        words_out[piece, :, :width] = join(first, second)
        words_out[piece, :, width : width + half] = join(linear[:, :half], linear[:, half:])
        pick = lax.broadcasted_iota(jnp.int32, (part, 128), 1)
        words_out[piece, :, width + half :] = jnp.where(
            pick == 0, linear_units, jnp.where(pick == 1, first_units, second_units)
        )
        shipped(piece, o).start()

    def decode(piece, rows):
        units = words_in[piece, :, width + half :].astype(jnp.float32) * (1.0 / (FULL * UNIT))
        left, right = split(words_in[piece, :, width : width + half])
        sums[0, rows, :half] += left.astype(jnp.float32) * units[:, 0:1]
        sums[0, rows, half:] += right.astype(jnp.float32) * units[:, 0:1]
        first, second = split(words_in[piece, :, :width])
        sums[1, rows] += first.astype(jnp.float32) * units[:, 1:2]
        sums[2, rows] += second.astype(jnp.float32) * units[:, 2:3]

    whole, low, high = pl.ds(0, owned), pl.ds(0, part), pl.ds(part, part)

    swapped(order[0]).wait_recv()
    for cols in tiles:
        first_hilbert[:, cols] = transform(order[0], whole, cols)

    for o in range(1, peers + 1):
        told(o).wait_recv()
    stats = stat_out[...]
    for o in range(peers):
        stats = stats + stat_in[o]
    weight = lax.rsqrt(stats[:, :128] / (lag_count * jnp.maximum(stats[:, 128:], 1.0)) + 0.1)
    weight = jnp.where(core == 0, weight, jnp.concatenate([weight[days:], weight[:days]], axis=0))
    for d in range(all_days):
        day_weight[d] = jnp.broadcast_to(weight[d : d + 1, :1], (owned, 1))

    for cols in tiles:
        add_days(order[0], whole, cols, first_hilbert[:, cols])
    encode(0, low, 1)
    encode(1, high, 2)

    def far_block(step, carry):
        o = chips - 1 - step
        swapped(chip ^ o).wait_recv()
        for cols in tiles:
            add_days(chip ^ o, whole, cols, transform(chip ^ o, whole, cols))
        encode(2 * o - 2, low, o)
        encode(2 * o - 1, high, o)
        return carry

    if chips > 4:
        lax.fori_loop(0, chips - 4, far_block, 0)

    def near_half(q, carry):
        o = 1 + q % 2
        g = chip ^ o
        here = pl.ds(pl.multiple_of(((q + q // 2) % 2) * part, part), part)

        @pl.when(q < 2)
        def _():
            swapped(g).wait_recv()

        for cols in tiles:
            add_days(g, here, cols, transform(g, here, cols))

        @pl.when(q >= 2)
        def _():
            shipped(3 - q, o).wait_recv()
            decode(3 - q, low)

        encode(2 + q, low, o)
        return carry

    lax.fori_loop(0, 4, near_half, 0)
    swapped(chip).wait_recv()
    for cols in tiles:
        add_days(chip, whole, cols, transform(chip, whole, cols))

    def arrive(piece, carry):
        turn = piece + jnp.where(piece // 2 == 2, 1, 0)
        shipped(piece, 1).wait_recv()
        decode(piece, pl.ds(pl.multiple_of((turn % 2) * part, part), part))
        return carry

    lax.fori_loop(2, pieces, arrive, 0)
    real, imag = sums[1, :, :lag_count], sums[2, :, :lag_count]
    linear_ref[...] = sums[0, :, :lag_count]
    power_ref[...] = real * real + imag * imag

    mask_copy.wait_send()
    for g in range(chips):
        swapped(g).wait_send()
    for o in range(1, peers + 1):
        told(o).wait_send()
    for piece in range(pieces):
        shipped(piece, 1).wait_send()


def general_sums(correlations, mask):
    days, pairs, lag_count = correlations.shape
    groups = lax.axis_size("day")
    chips = groups // 2
    owned = pairs // groups
    width = padded(lag_count)
    peers = 2 * lax.axis_size("pair") - 1

    strip = jnp.asarray(kernel_strip(lag_count))
    size = width + width // 2 + 128
    pieces = 2 * chips - 2
    out = jax.ShapeDtypeStruct((owned, lag_count), jnp.float32)
    vmem = pl.BlockSpec(memory_space=pltpu.VMEM)
    hbm = pl.BlockSpec(memory_space=pl.ANY)
    dma = pltpu.SemaphoreType.DMA
    return pl.pallas_call(
        functools.partial(stack_kernel, lag_count),
        in_specs=[hbm, vmem, hbm],
        out_specs=(vmem, vmem),
        out_shape=(out, out),
        scratch_shapes=[
            pltpu.VMEM((chips, 2 * days, owned, lag_count), jnp.bfloat16),
            pltpu.VMEM((chips, days, owned, lag_count), jnp.bfloat16),
            pltpu.VMEM(strip.shape, jnp.bfloat16),
            pltpu.VMEM((width, width), jnp.bfloat16),
            pltpu.VMEM((3, owned, width), jnp.float32),
            pltpu.VMEM((2 * days * owned, width), jnp.float32),
            pltpu.VMEM((days, pairs), jnp.int32),
            pltpu.VMEM((pairs, 2 * days), jnp.float32),
            pltpu.VMEM((chips, 2 * days, owned, 1), jnp.float32),
            pltpu.VMEM((2 * days, owned, 1), jnp.float32),
            pltpu.VMEM((2 * days, 256), jnp.float32),
            pltpu.VMEM((peers, 2 * days, 256), jnp.float32),
            pltpu.VMEM((pieces, owned // 2, size), jnp.int32),
            pltpu.VMEM((pieces, owned // 2, size), jnp.int32),
            dma((chips,)), dma((chips,)), dma, dma((chips,)), dma((chips,)), dma, dma,
            dma((peers,)), dma((peers,)), dma((pieces,)), dma((pieces,)),
        ],
        compiler_params=pltpu.CompilerParams(
            vmem_limit_bytes=46 * 2**20, collective_id=0, has_side_effects=True
        ),
        name="stack",
    )(correlations.reshape(days, groups, owned, lag_count), mask, strip)


LANES = 128
CHUNK = 512
HALF = CHUNK // 2
ROWS = HALF // 2
WORDS = ROWS + ROWS // 2
PACK = WORDS + 8
SENT = WORDS + 3


def block_strip(lag_count):
    f32 = np.float32
    offset = np.arange(lag_count, dtype=np.int32)
    offset = np.where(offset > lag_count // 2, offset - lag_count, offset)
    angle = f32(np.pi) * offset.astype(f32) / f32(lag_count)
    parity = f32(1) - f32(2) * (offset % 2).astype(f32)
    sine = np.where(offset == 0, f32(1), np.sin(angle)).astype(f32)
    kernel = np.where(offset == 0, f32(0), (np.cos(angle) - parity) / (f32(lag_count) * sine))
    width = chunked(lag_count)
    index = np.arange(TILE)[:, None] - np.arange(2 * width - TILE)[None, :] + (width - TILE)
    return kernel.astype(f32)[index % lag_count].astype(jnp.bfloat16)


def chunked(lag_count):
    return -(-lag_count // CHUNK) * CHUNK


def sorting_matrix(rows):
    lags = TILE // rows
    out = np.arange(TILE)
    source = (out % lags) * rows + out // lags
    return (source[:, None] == np.arange(TILE)[None, :]).astype(jnp.bfloat16)


def fast_kernel(
    lag_count, x_hbm, mask_hbm, counts_hbm, strip_hbm, sorter_hbm, power_ref, linear_ref, inverse_ref,
    mask_ref, counts_ref, sorter, raw, own, theirs, strip, even_h, odd_h, sums, scale, bias, mask_in, stat_out, stat_in,
    coded, parts, partial_in, relay_out, final_in, total,
    load_sem, small_sem, swap_send, swap_recv, late_send, late_recv, mask_send, mask_recv, stat_send, stat_recv,
    partial_send, partial_recv, final_send, final_recv, own_send, own_recv,
):
    f32 = jnp.float32
    width = raw.shape[0]
    planes = raw.shape[1]
    loads = width // TILE
    chunks = width // CHUNK
    steps = 2 * chunks
    peers = stat_in.shape[0]
    days = mask_ref.shape[0]
    tiles = mask_ref.shape[1] // LANES
    lags = TILE // planes
    me, plane = lax.axis_index("day"), lax.axis_index("pair")
    chip, core = me // 2, me % 2
    partner = {"day": me ^ 1, "pair": plane}

    def pick(s, table):
        return sum(jnp.where(s == i, value, 0) for i, value in enumerate(table))

    def order(s):
        return (
            jnp.where(core == 0, pick(s, (0, 0, 0, 1, 0, 1, 1, 1)), s // chunks),
            jnp.where(core == 0, pick(s, (0, 1, 2, 0, 3, 1, 2, 3)), pick(s, (3, 2, 1, 0, 0, 1, 2, 3))),
        )

    def near_step(k):
        return jnp.where(core == 0, pick(k, (3, 5, 6, 7)), pick(k, (3, 2, 1, 0)))

    def route(k, half):
        return pick(2 * k + half, (0, 0, 0, 1, 0, 1, 1, 1)), pick(2 * k + half, (0, 1, 2, 0, 3, 1, 2, 3))

    def near(o, c):
        return {"day": 2 * (chip ^ o) + c, "pair": plane}

    def peer(o):
        rank = (2 * plane + core + o) % (peers + 1)
        return {"day": 2 * chip + rank % 2, "pair": rank // 2}

    def loaded(j, count=TILE):
        rows = pl.ds(j * TILE, count)
        return pltpu.make_async_copy(x_hbm.at[rows], raw.at[rows], load_sem.at[j])

    def remote(source, target, send, recv, device):
        return pltpu.make_async_remote_copy(
            source, target, send, recv, device_id=device, device_id_type=MESH
        )

    def mine(slot):
        return 2 * (1 - core) + 1 - slot

    def swapped(j):
        rows = pl.ds(pl.multiple_of(j * TILE, TILE), TILE)
        return remote(
            own.at[2 * core + 1, :, rows], theirs.at[0, :, rows], swap_send.at[j], swap_recv.at[j], partner
        )

    def swapped_late():
        return remote(own.at[2 * core], theirs.at[1], late_send, late_recv, partner)

    def told(o):
        return remote(stat_out, stat_in.at[o - 1], stat_send.at[o - 1], stat_recv.at[o - 1], peer(o))

    sent = pl.ds(0, SENT)

    def relayed(s, k, half):
        far, j = route(k, half)
        return remote(
            coded.at[s, half, :, sent], partial_in.at[j, :, sent], partial_send.at[k, half], partial_recv.at[j],
            near(2 - far, 1 - far),
        )

    def finished(source, k, half, c):
        return remote(
            source.at[sent], final_in.at[1 - core, k, half, sent], final_send.at[k, half, c],
            final_recv.at[1 - core, k, half], near(2 - core, c),
        )

    def handed(s, k, half):
        return remote(
            parts.at[s, half, 0], total.at[k, half], own_send.at[k, half], own_recv.at[k, half], partner
        )

    last = loads - 1
    small = [
        pltpu.make_async_copy(source, target, small_sem.at[i])
        for i, (source, target) in enumerate(
            ((sorter_hbm, sorter), (mask_hbm, mask_ref), (counts_hbm, counts_ref), (strip_hbm, strip))
        )
    ]
    for copy in small[:3]:
        copy.start()
    for j in range(last):
        loaded(j).start()
    loaded(last, lag_count - last * TILE).start()
    small[3].start()
    barrier = pltpu.get_barrier_semaphore()
    for o in range(1, peers + 1):
        pl.semaphore_signal(barrier, inc=1, device_id=peer(o), device_id_type=MESH)
    for o in (1, 2):
        for c in (0, 1):
            pl.semaphore_signal(barrier, inc=1, device_id=near(o, c), device_id_type=MESH)
    raw[lag_count:] = jnp.zeros((width - lag_count, planes, LANES), raw.dtype)
    pl.semaphore_wait(barrier, peers + 4)
    small[0].wait()
    small[1].wait()
    mask_copy = remote(mask_ref, mask_in, mask_send, mask_recv, partner)
    mask_copy.start()

    def sort(j, energy):
        energy = [energy[i] for i in range(planes)]
        for g in range(TILE // (2 * lags)):
            at = pl.multiple_of(j * TILE + g * 2 * lags, 2 * lags)
            pair = [raw[pl.ds(at + h * lags, lags)].reshape(TILE, LANES) for h in (0, 1)]
            out = jnp.dot(sorter[...], jnp.concatenate(pair, axis=1), preferred_element_type=f32)
            for t in range(tiles):
                for d in range(days):
                    i = t * days + d
                    lane = (d % 2) * LANES
                    for h in (0, 1):
                        value = out[i * lags : (i + 1) * lags, h * LANES : (h + 1) * LANES]
                        energy[i] = energy[i] + jnp.sum((value * value).reshape(-1, 8, LANES), axis=0)
                        own[chip ^ t, d // 2, pl.ds(at + h * lags, lags), lane : lane + LANES] = value.astype(own.dtype)
        return jnp.stack(energy)

    def sort_load(j, energy):
        loaded(j).wait()
        energy = sort(j, energy)
        swapped(j).start()
        return energy

    energy = lax.fori_loop(0, last, sort_load, jnp.zeros((planes, 8, LANES), f32))
    loaded(last, lag_count - last * TILE).wait()
    energy = sort(last, energy)
    swapped(last).start()
    swapped_late().start()

    found, used = [], []
    for d in range(days):
        rows = [mask_ref[d : d + 1, t * LANES : (t + 1) * LANES].astype(f32) for t in range(tiles)]
        one = sum(jnp.sum(energy[t * days + d], axis=0, keepdims=True) * rows[t] for t in range(tiles))
        found.append(one)
        used.append(sum(rows))
    stat_out[...] = jnp.concatenate(found + used, axis=0)
    for o in range(1, peers + 1):
        told(o).start()

    def operand(slot, dp):
        return own[mine(slot), dp] if dp < days // 2 else theirs[slot, dp - days // 2]

    parts_of = CHUNK // TILE

    def transform_piece(slot, k, piece, target):
        dp, part = piece // parts_of, piece % parts_of
        start = pl.multiple_of(width - TILE - (k * parts_of + part) * TILE, TILE)
        target[part * TILE : (part + 1) * TILE, dp * TILE : (dp + 1) * TILE] = jnp.dot(
            strip[:, pl.ds(start, width)], operand(slot, dp), preferred_element_type=f32
        )

    def transform(slot, k, pieces, target):
        for piece in pieces:
            transform_piece(slot, k, piece, target)

    def add_days(slot, k, first, stop, source):
        size = 32
        for row in range(first, stop, size):
            at = pl.multiple_of(k * CHUNK + row, size)
            lin = one = two = jnp.zeros((size // 8, 8, LANES), f32)
            for e in range(2 * days):
                dp, lane = e // 2, (e % 2) * LANES
                if e < days:
                    x = own[mine(slot), dp, pl.ds(at, size), lane : lane + LANES]
                else:
                    x = theirs[slot, dp - days // 2, pl.ds(at, size), lane : lane + LANES]
                x = x.astype(f32).reshape(size // 8, 8, LANES)
                h = source[row : row + size, e * LANES : (e + 1) * LANES].reshape(size // 8, 8, LANES)
                r = lax.rsqrt(x * x + h * h + bias[slot, e][None])
                lin = lin + x * scale[slot, e][None]
                one = one + x * r
                two = two + h * r
            for v, value in enumerate((lin, one, two)):
                sums[v, row : row + size] = value.reshape(size, LANES)

    low_lane = lax.broadcasted_iota(jnp.int32, (ROWS, LANES), 1) < LANES // 2

    def split(half, v, c):
        a = sums[v, half * HALF : half * HALF + ROWS]
        b = sums[v, half * HALF + ROWS : (half + 1) * HALF]
        if c == 0:
            return jnp.where(low_lane, a, pltpu.roll(b, LANES // 2, 1))
        return jnp.where(low_lane, pltpu.roll(a, LANES // 2, 1), b)

    def encode(target, values):
        codes_of, units = [], []
        for value in values:
            top = jnp.max(jnp.abs(value), axis=0, keepdims=True)
            unit = (top * UNIT).astype(jnp.int32) + 1
            step = FULL * UNIT / unit.astype(f32)
            codes_of.append((value * step + 32768.5).astype(jnp.int32))
            units.append(unit)
        lin, one, two = codes_of
        target[:ROWS] = one * 65536 + two
        target[ROWS:WORDS] = lin[: ROWS // 2] * 65536 + lin[ROWS // 2 :]
        pick = lax.broadcasted_iota(jnp.int32, (8, LANES), 0)
        target[WORDS:] = jnp.where(pick == 0, units[0], jnp.where(pick == 1, units[1], units[2]))

    def decode(source):
        units = source[WORDS:].astype(f32) * (1.0 / (FULL * UNIT))

        def value(code, v):
            return (code.astype(f32) - 32768.0) * units[v : v + 1]

        def pieces(word):
            return lax.shift_right_logical(word, jnp.full_like(word, 16)), word & 65535

        one, two = pieces(source[:ROWS])
        top, bottom = pieces(source[ROWS:WORDS])
        return (jnp.concatenate([value(top, 0), value(bottom, 0)], axis=0), value(one, 1), value(two, 2))

    def code(s, half, c):
        values = [split(half, v, c) for v in range(3)]
        for v in range(3):
            parts[s, half, c, v] = values[v]
        encode(coded.at[s, half, c], values)

    def step_both(s, source, target):
        slot, k = order(s)
        rows = (0, 128, 256, 384, CHUNK)
        for piece in range(2 * days):
            if piece < len(rows) - 1:
                add_days(slot, k, rows[piece], rows[piece + 1], source)
            if piece in (2, 3):
                code(s, 0, piece - 2)
            if piece in (4, 5):
                code(s, 1, piece - 4)
            if target is not None:
                transform_piece(*order(s + 1), piece, target)

    def send(s, halves=(0, 1)):
        slot, k = order(s)

        for half in halves:
            @pl.when(jnp.logical_and(slot + core == 1, route(k, half)[0] == core))
            def _():
                for c in (0, 1):
                    finished(coded.at[s, half, c], k, half, c).start()

        @pl.when(slot + core == 0)
        def _():
            for half in halves:
                relayed(s, k, half).start()

        @pl.when(slot + core == 2)
        def _():
            for half in halves:
                handed(s, k, half).start()

    def relay(j):
        k = jnp.where(core == 0, pick(j, (1, 2, 3, 3)), pick(j, (0, 0, 1, 2)))
        half = jnp.where(core == 0, pick(j, (1, 1, 0, 1)), pick(j, (0, 1, 0, 0)))
        s = near_step(k)
        remote(
            coded.at[0, 0, :, sent], partial_in.at[j, :, sent], partial_send.at[0, 0], partial_recv.at[j], partner
        ).wait_recv()
        for c in (0, 1):
            far = decode(partial_in.at[j, c])
            encode(relay_out.at[j, c], [parts[s, half, c, v] + far[v] for v in range(3)])
            finished(relay_out.at[j, c], k, half, c).start()

    small[3].wait()
    transform(*order(0), range(days), even_h)
    for j in range(loads):
        swapped(j).wait_recv()
    transform(*order(0), range(days, 2 * days), even_h)
    transform(*order(1), range(2 * days), odd_h)

    mask_copy.wait_recv()
    for o in range(1, peers + 1):
        told(o).wait_recv()
    ours, other = stat_out[...], jnp.zeros_like(stat_out)
    for o in range(1, peers + 1):
        if o % 2:
            other = other + stat_in[o - 1]
        else:
            ours = ours + stat_in[o - 1]
    for which, stats in enumerate((ours, other)):
        row = jnp.sum(stats, axis=1, keepdims=True)
        power = row[:days] / (lag_count * jnp.maximum(row[days:], 1.0)) + 0.1
        weight = lax.rsqrt(power)
        for slot in (0, 1):
            at = pl.multiple_of((chip ^ mine(slot)) * LANES, LANES)
            usable = (mask_in if which else mask_ref)[:, pl.ds(at, LANES)].astype(f32)
            by_day = weight * usable
            offset = jnp.where(usable > 0.0, 0.25 * power, jnp.inf)
            for d in range(days):
                scale[slot, which * days + d] = jnp.broadcast_to(by_day[d : d + 1], (8, LANES))
                bias[slot, which * days + d] = jnp.broadcast_to(offset[d : d + 1], (8, LANES))
    for half in (0, 1):
        add_days(*order(0), half * HALF, half * HALF + HALF, even_h)
        code(0, half, 0)
        code(0, half, 1)
        send(0, (half,))
    swapped_late().wait_recv()

    def step(i, carry):
        for s, target, source in ((2 * i + 1, even_h, odd_h), (2 * i + 2, odd_h, even_h)):
            step_both(s, source, target)
            send(s)
            if source is odd_h:
                @pl.when(jnp.logical_and(core == 1, i == 1))
                def _():
                    lax.fori_loop(0, 2, lambda j, carry: (relay(j), carry)[1], 0)

                @pl.when(i == 2)
                def _():
                    relay(3 * core)
            else:
                @pl.when(i + core == 2)
                def _():
                    relay(1 + core)
        return carry

    lax.fori_loop(0, chunks - 1, step, 0)
    step_both(steps - 1, odd_h, None)
    send(steps - 1)

    @pl.when(core == 0)
    def _():
        lax.fori_loop(2, chunks, lambda j, carry: (relay(j), carry)[1], 0)

    small[2].wait()
    inverse_ref[...] = 1.0 / jnp.maximum(counts_ref[...].astype(f32), 1.0)

    @pl.when(core == 0)
    def _():
        for k in range(chunks):
            for half in (0, 1):
                handed(0, k, half).wait_recv()

    @pl.when(core == 1)
    def _():
        def keep(k, carry):
            for half in (0, 1):
                for v in range(3):
                    total[k, half, v] = parts[chunks + k, half, 1, v]
            return carry

        lax.fori_loop(0, chunks, keep, 0)

    def settle():
        mask_copy.wait_send()
        swapped_late().wait_send()
        for j in range(loads):
            swapped(j).wait_send()
        for o in range(1, peers + 1):
            told(o).wait_send()
        for k in range(chunks):
            for half in (0, 1):
                for c in (0, 1):
                    finished(relay_out.at[0, 0], k, half, c).wait_send()

            @pl.when(core == 0)
            def _():
                for half in (0, 1):
                    relayed(0, k, half).wait_send()

            @pl.when(core == 1)
            def _():
                for half in (0, 1):
                    handed(0, k, half).wait_send()

    seen = set()
    arrivals = (
        (0, 3, 0), (0, 3, 1), (0, 2, 1), (0, 1, 1), (1, 0, 0), (1, 0, 1), (0, 0, 0), (0, 0, 1),
        (1, 1, 0), (0, 1, 0), (1, 1, 1), (0, 2, 0), (1, 2, 0), (1, 2, 1), (1, 3, 0), (1, 3, 1),
    )
    for s, k, half in arrivals:
        if (s, k, half) == (1, 3, 0):
            settle()
        remote(
            relay_out.at[0, 0, sent], final_in.at[s, k, half, sent], final_send.at[k, half, 0],
            final_recv.at[s, k, half], partner,
        ).wait_recv()
        found = decode(final_in.at[s, k, half])
        if (k, half) not in seen:
            seen.add((k, half))
            for v in range(3):
                total[k, half, v] += found[v]
            continue
        lin, one, two = (total[k, half, v] + found[v] for v in range(3))
        for ref, value in ((linear_ref, lin), (power_ref, one * one + two * two)):
            turned = value.T
            for part in (0, 1):
                start = k * CHUNK + half * HALF + part * ROWS
                stop = min(start + ROWS, lag_count)
                if stop > start:
                    rows = turned[part * LANES // 2 : (part + 1) * LANES // 2]
                    ref[:, start:stop] = rows[:, : stop - start]


def fast_stack(correlations, mask, counts):
    days, pairs, lag_count = correlations.shape
    owned = pairs // lax.axis_size("day")
    peers = 2 * lax.axis_size("pair") - 1
    tiles = pairs // LANES
    planes = tiles * days
    width = chunked(lag_count)
    chunks, loads = width // CHUNK, width // TILE
    by_lag = correlations.transpose(2, 0, 1).reshape(lag_count, days, tiles, LANES)
    by_lag = by_lag.transpose(0, 2, 1, 3).reshape(lag_count, planes, LANES)
    strip = jnp.asarray(block_strip(lag_count))
    sorter = jnp.asarray(sorting_matrix(planes))
    out = jax.ShapeDtypeStruct((owned, lag_count), jnp.float32)
    vmem = pl.BlockSpec(memory_space=pltpu.VMEM)
    hbm = pl.BlockSpec(memory_space=pltpu.HBM)
    dma = pltpu.SemaphoreType.DMA
    bf16, f32, i32 = jnp.bfloat16, jnp.float32, jnp.int32
    power, linear_sum, inverse = pl.pallas_call(
        functools.partial(fast_kernel, lag_count),
        in_specs=[hbm] * 5,
        out_specs=(vmem, vmem, vmem),
        out_shape=(out, out, jax.ShapeDtypeStruct((1, owned), f32)),
        scratch_shapes=[
            pltpu.VMEM(mask.shape, i32),
            pltpu.VMEM((1, owned), i32),
            pltpu.VMEM(sorter.shape, bf16),
            pltpu.VMEM((width, planes, LANES), bf16),
            pltpu.VMEM((tiles, days // 2, width, TILE), bf16),
            pltpu.VMEM((2, days // 2, width, TILE), bf16),
            pltpu.VMEM(strip.shape, bf16),
            pltpu.VMEM((CHUNK, 2 * days * LANES), f32),
            pltpu.VMEM((CHUNK, 2 * days * LANES), f32),
            pltpu.VMEM((3, CHUNK, LANES), f32),
            pltpu.VMEM((2, 2 * days, 8, LANES), f32),
            pltpu.VMEM((2, 2 * days, 8, LANES), f32),
            pltpu.VMEM(mask.shape, i32),
            pltpu.VMEM((2 * days, LANES), f32),
            pltpu.VMEM((peers, 2 * days, LANES), f32),
            pltpu.VMEM((2 * chunks, 2, 2, PACK, LANES), i32),
            pltpu.VMEM((2 * chunks, 2, 2, 3, ROWS, LANES), f32),
            pltpu.VMEM((chunks, 2, PACK, LANES), i32),
            pltpu.VMEM((chunks, 2, PACK, LANES), i32),
            pltpu.VMEM((2, chunks, 2, PACK, LANES), i32),
            pltpu.VMEM((chunks, 2, 3, ROWS, LANES), f32),
            dma((loads,)), dma((4,)), dma((loads,)), dma((loads,)), dma, dma, dma, dma, dma((peers,)), dma((peers,)),
            dma((chunks, 2)), dma((chunks,)), dma((chunks, 2, 2)), dma((2, chunks, 2)),
            dma((chunks, 2)), dma((chunks, 2)),
        ],
        compiler_params=pltpu.CompilerParams(
            vmem_limit_bytes=46 * 2**20, collective_id=0, has_side_effects=True
        ),
        name="stack",
    )(*(pltpu.with_memory_space_constraint(v, pltpu.HBM) for v in (by_lag, mask, counts.reshape(1, owned), strip, sorter)))
    return linear_sum, power, inverse.reshape(owned, 1)


def shards(correlations, mask, counts):
    days, pairs, lag_count = correlations.shape
    groups = lax.axis_size("day")
    four = groups == 8 and days == 4 and chunked(lag_count) == 4 * CHUNK
    if four and pairs == 4 * LANES:
        linear_sum, power, inverse = fast_stack(correlations, mask, counts)
    else:
        linear_sum, power = general_sums(correlations, mask)
        inverse = (1.0 / jnp.maximum(counts.astype(jnp.float32), 1.0))[:, None]
    linear = linear_sum * inverse
    return (linear * (power * (inverse * inverse)), linear)


def solution(mesh):
    placed = (P("day", "pair", None), P("day", "pair"), P(("pair", "day")))
    return jax.shard_map(
        shards,
        mesh=mesh,
        in_specs=placed,
        out_specs=(P(("pair", "day"), None), P(("pair", "day"), None)),
        check_vma=False,
    )
```
